32 devices in a mesh: expert: 16 (over z, y, x), dp: 2 (over core).
Axes of the slice: x: 2, y: 2, z: 4, core: 2. Of those that a mesh axis runs over, the one named last changes fastest.
Arguments:
- tokens: bfloat16 [4096, 1440], P(('expert', 'dp')), may hold values from -6 to 6
- cotangent: bfloat16 [4096, 1440], P(('expert', 'dp')), may hold values from -0.3984375 to 0.3984375
- expert_ids: int32 [4096, 4], P(('expert', 'dp')), may hold values from 0 to 15, all different within a row; in each aligned block of 128 rows (0 to 127, 128 to 255, ...) at most 48 rows name the same one
- gate_weights: float32 [4096, 4], P(('expert', 'dp')), may hold values from 0.05 to 1
- w_gate: bfloat16 [16, 1440, 1440], P('expert', 'dp'), may hold values from -0.15625 to 0.15625
- w_up: bfloat16 [16, 1440, 1440], P('expert', 'dp'), may hold values from -0.15625 to 0.15625
- w_down: bfloat16 [16, 1440, 1440], P('expert', 'dp'), may hold values from -0.15625 to 0.15625
Outputs:
- mixed: bfloat16 [4096, 1440], P(('expert', 'dp'))
- grad_gate: bfloat16 [16, 1440, 1440], P('expert', 'dp')
- grad_up: bfloat16 [16, 1440, 1440], P('expert', 'dp')
- grad_down: bfloat16 [16, 1440, 1440], P('expert', 'dp')
The draws below stay inside these ranges and needn't reach their ends.
Inputs may be any that keep to these rules, and one draw needn't show every extreme that they name: `expert_ids`: each row names 4 different experts. Within the rows of one device no expert is named more than 48 times, a bound that some block reaches.
All inputs are finite; a program needn't handle non-finite values.
Results may differ from the reference program's by a relative error of at most 0.013.
Values may be sent and summed in bfloat16 or wider, within the bound.
A program may use at most 128 MiB of HBM per device.

```python
import math
import jax
import jax.numpy as jnp
import numpy as np
from jax import lax

D = 1440
FH = 1440
TOPK = 4
TOK_DEV = 128
CAP = 512
EXPERTS = 16
SLOT = 48
TOKENS = 4096
N_EXPERT = 16
N_DP = 2


def shard_levels(key, dims, pieces, smallest, high):
    level = 1.0
    for dim, shards_of in pieces:
        draws = jax.random.uniform(jax.random.fold_in(jax.random.fold_in(key, 6), dim), (shards_of,), jnp.float32, smallest / len(pieces), high / len(pieces))
        level = level * jnp.repeat(jnp.exp(draws), dims[dim] // shards_of).reshape((-1,) + (1,) * (len(dims) - 1 - dim))
    return level


def routed_block(stream_key, own, number, rows, number_of, top, reach, skew):
    ranking = jax.random.permutation(stream_key, number_of)
    packed, usual = shares(number_of, rows * top, reach, skew, True), shares(number_of, rows * top, reach, skew, False)
    places = jnp.arange(number_of)

    def named(sizes, offset_by):
        used = int((sizes > 0).sum())
        fixed = max(1, used // 4)
        shifted = fixed + (places - fixed + offset_by * (used - fixed)) % max(1, number_of - fixed)
        return jnp.zeros((number_of,), jnp.int32).at[ranking[jnp.where(places < fixed, places, shifted)]].set(jnp.asarray(sizes, jnp.int32))

    sizes = jnp.where(number % 4 == 0, named(packed, number // 4), named(usual, number - number // 4 - 1))
    mixed = jax.random.permutation(jax.random.fold_in(own, 3), number_of)
    giver, receiver = mixed[0:number_of // 2 * 2:2], mixed[1:number_of // 2 * 2:2]
    margin = jnp.minimum(sizes[giver] - 1, reach - sizes[receiver]) // 2
    margin = jnp.where((giver == ranking[0]) | (receiver == ranking[0]) | (sizes[receiver] == 0), 0, jnp.maximum(margin, 0))
    shifted = jax.random.randint(jax.random.fold_in(own, 4), (number_of // 2,), 0, 1 << 20) % (margin + 1)
    sizes = sizes.at[giver].add(-shifted).at[receiver].add(shifted)
    items = jnp.searchsorted(jnp.cumsum(sizes), jnp.arange(rows * top), side="right").astype(jnp.int32)
    listing = items.reshape(top, rows).T
    listing = listing[jax.random.permutation(jax.random.fold_in(own, 1), rows)]
    offset_by = jax.random.randint(jax.random.fold_in(own, 2), (rows, 1), 0, top)
    return jnp.take_along_axis(listing, (jnp.arange(top)[None, :] + offset_by) % top, axis=1)


def shares(count, total, bound, skew, full):
    weights = [(1 << 20) // math.isqrt(rank ** skew) + 1 for rank in range(1, count + 1)]
    largest = bound if full else min(bound, max(-(-total // count), total * weights[0] // sum(weights)))
    least = 1 if total - largest >= count - 1 else 0
    holding, rest = [largest] + [least] * (count - 1), total - largest - least * (count - 1)
    while rest > 0:
        candidates = [i for i in range(1, count) if holding[i] < largest] or [i for i in range(1, count) if holding[i] < bound]
        pool, left = sum([weights[i] for i in candidates]), rest
        for i in candidates:
            extra = min(bound - holding[i], max(1, left * weights[i] // pool), rest)
            holding[i] = holding[i] + extra
            rest = rest - extra
    return np.array(holding)


def centred(own_key, extent, scale, reach, split=(), kind=jnp.bfloat16):
    entries = scale * jax.random.normal(own_key, extent, jnp.float32)
    if split:
        entries = entries * shard_levels(own_key, extent, split, -0.22, 0.18)
    return jnp.clip(entries, -reach, reach).astype(kind)


def setup_inputs(seed: int = 0) -> dict:
    splits = jax.random.split(jax.random.key(seed), 8)
    tokens = centred(splits[0], (TOKENS, D), 1.0, 6.0, ((0, 32),))
    cotangent = centred(splits[1], (TOKENS, D), 0.05, 0.3984375, ((0, 32),))
    expert_ids_keys = jax.random.split(jax.random.fold_in(splits[2], 1), TOKENS // TOK_DEV)
    expert_ids_turns = jax.random.permutation(jax.random.fold_in(splits[2], 3), TOKENS // TOK_DEV)
    expert_ids = jax.vmap(lambda own, number: routed_block(jax.random.fold_in(splits[2], 2), own, number, TOK_DEV, EXPERTS, TOPK, SLOT, 2))(expert_ids_keys, expert_ids_turns).reshape((TOKENS, TOPK))
    gate_weights = jnp.clip(jnp.exp(math.log(1.0) - 2.9957323 * jax.random.uniform(splits[3], (TOKENS, TOPK), jnp.float32) ** shard_levels(splits[3], (TOKENS, TOPK), ((0, 32),), -0.2, 0.2)), 0.05, 1.0)
    w_gate = centred(splits[4], (EXPERTS, D, FH), D ** -0.5, 0.15625, ((0, 16), (1, 2)))
    w_up = centred(splits[5], (EXPERTS, D, FH), D ** -0.5, 0.15625, ((0, 16), (1, 2)))
    w_down = centred(splits[6], (EXPERTS, D, FH), FH ** -0.5, 0.15625, ((0, 16), (1, 2)))
    return dict(tokens=tokens, cotangent=cotangent, expert_ids=expert_ids, gate_weights=gate_weights, w_gate=w_gate, w_up=w_up, w_down=w_down)


SWISH_SLOPE = 1.702


def expert_pass(packed_x, packed_g, gate_mat, up_mat, down_mat):
    pre_gate = jnp.dot(packed_x, gate_mat, preferred_element_type=jnp.float32)
    pre_up = jnp.dot(packed_x, up_mat, preferred_element_type=jnp.float32)
    sigmoid_part = jax.nn.sigmoid(SWISH_SLOPE * pre_gate)
    value = pre_gate * sigmoid_part
    slope_term = sigmoid_part + SWISH_SLOPE * pre_gate * sigmoid_part * (1.0 - sigmoid_part)
    hidden = (value * (pre_up + 1.0)).astype(jnp.bfloat16)
    expert_out = jnp.dot(hidden, down_mat.T, preferred_element_type=jnp.float32).astype(jnp.bfloat16)
    d_hidden = jnp.dot(packed_g, down_mat, preferred_element_type=jnp.float32)
    grad_down = jnp.dot(packed_g.T, hidden, preferred_element_type=jnp.float32)
    d_gate = (d_hidden * (pre_up + 1.0) * slope_term).astype(jnp.bfloat16)
    d_up = (d_hidden * value).astype(jnp.bfloat16)
    grad_gate = jnp.dot(packed_x.T, d_gate, preferred_element_type=jnp.float32)
    grad_up = jnp.dot(packed_x.T, d_up, preferred_element_type=jnp.float32)
    return expert_out, jnp.stack([grad_gate, grad_up, grad_down]).astype(jnp.bfloat16)


def reference(tokens, cotangent, expert_ids, gate_weights, w_gate, w_up, w_down):
    assigns = TOK_DEV * TOPK
    expert_table = jnp.arange(EXPERTS, dtype=jnp.int32)

    def rank_block(block):
        onehot = (block[:, None] == expert_table[None, :]).astype(jnp.int32)
        local_rank = jnp.sum((jnp.cumsum(onehot, axis=0) - onehot) * onehot, axis=1)
        return local_rank, jnp.sum(onehot, axis=0)

    local_rank, block_counts = lax.map(rank_block, expert_ids.reshape(N_EXPERT * N_DP, assigns))
    local_rank = local_rank.reshape(N_EXPERT, N_DP, assigns)
    block_counts = block_counts.reshape(N_EXPERT, N_DP, EXPERTS)
    offsets = jnp.cumsum(block_counts, axis=0) - block_counts
    group_ids = expert_ids.reshape(N_EXPERT, N_DP, assigns)
    position = jnp.take_along_axis(offsets, group_ids, axis=2) + local_rank
    target = jnp.where(position < CAP, position, CAP).astype(jnp.int32)
    gates = gate_weights.reshape(N_EXPERT, N_DP, assigns)
    token_rows = tokens.reshape(N_EXPERT, N_DP, TOK_DEV, D)
    cot_rows = cotangent.reshape(N_EXPERT, N_DP, TOK_DEV, D)
    inputs = (jnp.swapaxes(group_ids, 0, 1), jnp.swapaxes(target, 0, 1), jnp.swapaxes(gates, 0, 1),
              jnp.swapaxes(token_rows, 0, 1), jnp.swapaxes(cot_rows, 0, 1))

    def run_expert(item):
        return expert_pass(item[0], item[1], item[2], item[3], item[4])

    def per_group(totals, group):
        ids_here, target_here, gates_here, tokens_here, cot_here = group
        token_copies = jnp.repeat(tokens_here, TOPK, axis=1)
        gated = (gates_here[:, :, None] * jnp.repeat(cot_here, TOPK, axis=1).astype(jnp.float32)).astype(jnp.bfloat16)
        packed_x = jnp.zeros((EXPERTS, CAP, D), jnp.bfloat16).at[ids_here, target_here].set(token_copies, mode="drop")
        packed_g = jnp.zeros((EXPERTS, CAP, D), jnp.bfloat16).at[ids_here, target_here].set(gated, mode="drop")
        outputs, group_grads = lax.map(run_expert, (packed_x, packed_g, w_gate, w_up, w_down))
        group_grads = lax.optimization_barrier(group_grads)
        totals = totals + group_grads.astype(jnp.float32)
        kept = (target_here < CAP).astype(jnp.float32)
        fetched = outputs[ids_here, jnp.minimum(target_here, CAP - 1)]
        weighted = (gates_here * kept)[:, :, None] * fetched.astype(jnp.float32)
        mixed_group = jnp.sum(weighted.reshape(N_EXPERT, TOK_DEV, TOPK, D), axis=2).astype(jnp.bfloat16)
        return totals, mixed_group

    totals = jnp.zeros((EXPERTS, 3, D, FH), jnp.float32)
    totals, mixed_all = lax.scan(per_group, totals, inputs)
    mixed = jnp.swapaxes(mixed_all, 0, 1).reshape(TOKENS, D)
    grads = totals.astype(jnp.bfloat16)
    return (mixed, grads[:, 0], grads[:, 1], grads[:, 2])
```

```python
import functools

import jax
import jax.numpy as jnp
from jax import lax
from jax.experimental import pallas as pl
from jax.experimental.pallas import tpu as pltpu
from jax.sharding import PartitionSpec as P


CAP = 512
INNER = 4
TILE = 512
SWISH_SLOPE = 1.702
F32 = jnp.float32
BF16 = jnp.bfloat16


def dot(a, b):
    return jnp.dot(a, b, preferred_element_type=F32)


def dot_nt(a, b):
    return lax.dot_general(a, b, (((1,), (1,)), ((), ())), preferred_element_type=F32)


def dot_tn(a, b):
    return lax.dot_general(a, b, (((0,), (0,)), ((), ())), preferred_element_type=F32)


def share_kernel(size, x_ref, all_ref, send_sem, recv_sem):
    me = lax.axis_index("expert")
    barrier = pltpu.get_barrier_semaphore()
    for k in range(1, size):
        pl.semaphore_signal(
            barrier, inc=1, device_id={"expert": lax.rem(me + k, size)},
            device_id_type=pl.DeviceIdType.MESH,
        )
    pl.semaphore_wait(barrier, size - 1)
    copies = []
    for k in range(1, size):
        copy = pltpu.make_async_remote_copy(
            src_ref=x_ref, dst_ref=all_ref.at[me],
            send_sem=send_sem.at[k], recv_sem=recv_sem.at[k],
            device_id={"expert": lax.rem(me + k, size)},
            device_id_type=pl.DeviceIdType.MESH,
        )
        copy.start()
        copies.append(copy)
    all_ref[me] = x_ref[...]
    for copy in copies:
        copy.wait()


def share(x):
    size = lax.axis_size("expert")
    return pl.pallas_call(
        functools.partial(share_kernel, size),
        out_shape=jax.ShapeDtypeStruct((size,) + x.shape, x.dtype),
        in_specs=[pl.BlockSpec(memory_space=pltpu.VMEM)],
        out_specs=pl.BlockSpec(memory_space=pltpu.VMEM),
        scratch_shapes=[
            pltpu.SemaphoreType.DMA((size,)),
            pltpu.SemaphoreType.DMA((size,)),
        ],
        compiler_params=pltpu.CompilerParams(collective_id=0, has_side_effects=True),
    )(x)


def layer(tokens, cotangent, expert_ids, gate_weights, w_gate, w_up, w_down):
    size = lax.axis_size("expert")
    rows, top = expert_ids.shape
    width = tokens.shape[1]
    slot = 3 * rows * top // (2 * size)
    inner = min(INNER, size)
    outer = size // inner
    me = lax.axis_index("expert")
    mine_out, mine_in = me // inner, me % inner
    half = outer // 2
    partner = jnp.bitwise_xor(mine_in, jnp.arange(inner, dtype=jnp.int32))

    def shift(x, by):
        pairs = [(d, (d // inner + by) % outer * inner + d % inner) for d in range(size)]
        return lax.ppermute(x, "expert", pairs)

    def gather_outer(x):
        blocks = [x] + [None] * (outer - 1)
        for r in range(1, half + 1):
            if outer > 1:
                blocks[r] = shift(blocks[r - 1], 1)
        for r in range(1, outer - half):
            blocks[outer - r] = shift(blocks[(outer - r + 1) % outer], -1)
        return blocks

    def exchange(blocks):
        moved = list(blocks)
        for d in range(inner - 1, 0, -1):
            pairs = [(e, e // inner * inner + (e % inner ^ d)) for e in range(size)]
            moved[d] = lax.ppermute(blocks[d], "expert", pairs)
        return jnp.concatenate(moved)

    def relay(blocks):
        held = jnp.concatenate(blocks)
        return exchange([dot(part, held).astype(BF16) for part in select])

    meta = jnp.concatenate([expert_ids.T.astype(F32), gate_weights.T], axis=0)
    meta_all = share(meta)
    meta_all, tokens = lax.optimization_barrier((meta_all, tokens))
    token_blocks = gather_outer(tokens)
    token_blocks, cotangent = lax.optimization_barrier((token_blocks, cotangent))
    cot_blocks = gather_outer(cotangent)

    ids_all = meta_all[:, :top, :].astype(jnp.int32)
    gates_all = meta_all[:, top:, :]
    back = (mine_out - jnp.arange(outer, dtype=jnp.int32)) % outer

    before = (jnp.arange(rows)[:, None] < jnp.arange(rows)[None, :]).astype(BF16)

    ids_relay = jnp.stack([
        lax.dynamic_index_in_dim(ids_all, back[r] * inner + mine_in, 0, keepdims=False)
        for r in range(outer)
    ])
    near = mine_out * inner + partner
    named = jnp.any(ids_relay[None] == near[:, None, None, None], axis=2)
    rank = dot(named.astype(BF16).reshape(inner * outer, rows), before)
    rank = rank.reshape(inner, outer, rows).astype(jnp.int32)
    place = jnp.where(named, rank, slot)
    hit = place[:, :, None, :] == jnp.arange(slot, dtype=jnp.int32)[None, None, :, None]
    same = jnp.eye(outer, dtype=jnp.bool_)
    select = (hit[:, :, :, None, :] & same[None, :, None, :, None]).astype(BF16)
    select = select.reshape(inner, outer * slot, outer * rows)

    mask = jnp.any(ids_all == me, axis=1)
    gate_of = jnp.sum(jnp.where(ids_all == me, gates_all, 0.0), axis=1)
    counts = jnp.sum(mask.astype(jnp.int32), axis=1)
    below = jnp.arange(size)[:, None] > jnp.arange(size)[None, :]
    starts = jnp.sum(jnp.where(below, counts[None, :], 0), axis=1)
    own_rank = dot(mask.astype(BF16), before).astype(jnp.int32)
    position = jnp.where(mask, starts[:, None] + own_rank, CAP).reshape(1, size * rows)
    row_index = jnp.arange(CAP, dtype=jnp.int32)
    row_gate = jnp.sum(
        jnp.where(position == row_index[:, None], gate_of.reshape(1, size * rows), 0.0),
        axis=1, keepdims=True,
    )
    source = back[None, :] * inner + partner[:, None]
    is_source = source[:, :, None] == jnp.arange(size, dtype=jnp.int32)
    slot_start = jnp.sum(jnp.where(is_source, starts, 0), axis=2)
    slot_live = jnp.sum(jnp.where(is_source, counts, 0), axis=2)
    within = jnp.arange(slot, dtype=jnp.int32)
    slot_row = jnp.where(
        within < slot_live[:, :, None], slot_start[:, :, None] + within, CAP
    ).reshape(1, inner * outer * slot)
    pack = (row_index[:, None] == slot_row).astype(BF16)

    full_gate, full_up, full_down = (
        lax.all_gather(w_gate, "dp", axis=1, tiled=True)[0],
        lax.all_gather(w_up, "dp", axis=1, tiled=True)[0],
        lax.all_gather(w_down, "dp", axis=1, tiled=True)[0],
    )

    recv_x = relay(token_blocks)
    packed_x = dot(pack, recv_x).astype(BF16)
    pre_gate = dot(packed_x, full_gate)
    pre_up = dot(packed_x, full_up)
    sig = jax.nn.sigmoid(SWISH_SLOPE * pre_gate)
    value = pre_gate * sig
    slope = sig + SWISH_SLOPE * pre_gate * sig * (1.0 - sig)
    hidden = (value * (pre_up + 1.0)).astype(BF16)
    out = (dot_nt(hidden, full_down) * row_gate).astype(BF16)
    spread = dot_tn(pack, out).astype(BF16).reshape(inner, outer * slot, width)

    recv_g = relay(cot_blocks)
    spread, recv_g = lax.optimization_barrier((spread, recv_g))
    returned = exchange([spread[d] for d in range(inner)])
    packed_g = (dot(pack, recv_g) * row_gate).astype(BF16)
    grad_down = dot_tn(packed_g, hidden).astype(BF16)
    d_hidden = dot(packed_g, full_down)
    d_gate = (d_hidden * (pre_up + 1.0) * slope).astype(BF16)
    d_up = (d_hidden * value).astype(BF16)
    returned, d_gate, d_up = lax.optimization_barrier((returned, d_gate, d_up))
    partial = dot_tn(select.reshape(inner * outer * slot, outer * rows), returned)
    partial = partial.reshape(outer, rows, width)
    partial, d_gate, d_up = lax.optimization_barrier((partial, d_gate, d_up))
    grad_gate = dot_tn(packed_x, d_gate).astype(BF16)
    grad_up = dot_tn(packed_x, d_up).astype(BF16)

    total = partial[0]
    ahead = partial[half]
    behind = partial[half + 1] if outer - half > 1 else None
    for r in range(half - 1, -1, -1):
        ahead = shift(ahead.astype(BF16), -1).astype(F32)
        if r > 0:
            ahead = ahead + partial[r]
    for r in range(half + 2, outer + 1):
        behind = shift(behind.astype(BF16), 1).astype(F32)
        if r < outer:
            behind = behind + partial[r]
    if half > 0:
        total = total + ahead
    if behind is not None:
        total = total + behind
    mixed = total.astype(BF16)

    grads = [
        lax.psum_scatter(g, "dp", scatter_dimension=0, tiled=True)[None]
        for g in (grad_down, grad_gate, grad_up)
    ]
    return mixed, grads[1], grads[2], grads[0]


def flip(i, d):
    out, bit = 0, 1
    while bit <= max(d, INNER - 1):
        out = out + lax.rem(lax.rem(i // bit, 2) + (d // bit) % 2, 2) * bit
        bit *= 2
    return out


def step_kernel(
    dims, tok_in, cot_in, meta_in, order_in, wg_in, wu_in, wd_in,
    mixed_out, gd_out, gg_out, gu_out,
    col, meta, sel, send, recv, back, pack, x, act, out, g, coef, w, xt, dact,
    zin, zout, near, mask, gq, start, count, place, row_gate,
    load_sem, z_send, z_recv, m_send, m_recv, ms_send, ms_recv, p_send, p_recv,
    w_send, w_recv, r_send, r_recv, g_send, g_recv, o_sem, free_sem,
):
    size, outer, inner, rows, width, top, slot, shard = dims
    span = inner * slot
    me = lax.axis_index("expert")
    dp = lax.axis_index("dp")
    mo, mi = me // inner, lax.rem(me, inner)
    pal = [flip(mi, d) + mo * inner for d in range(inner)]
    other = 1 - dp
    has_up, has_dn = mo < outer - 1, mo > 0
    mesh_id = pl.DeviceIdType.MESH

    def remote(src, dst, ss, rs, device):
        return pltpu.make_async_remote_copy(
            src_ref=src, dst_ref=dst, send_sem=ss, recv_sem=rs,
            device_id=device, device_id_type=mesh_id,
        )

    def tiles(fn):
        full = width // TILE
        if full:
            def step(i, carry):
                fn(pl.ds(pl.multiple_of(i * TILE, TILE), TILE))
                return carry

            lax.fori_loop(0, full, step, 0)
        if width % TILE:
            fn(pl.ds(full * TILE, width % TILE))

    own_rows = pl.ds(pl.multiple_of(dp * shard, 16), shard)
    loads = [
        pltpu.make_async_copy(tok_in, col.at[0, mo], load_sem.at[0]),
        pltpu.make_async_copy(cot_in, col.at[1, mo], load_sem.at[1]),
        pltpu.make_async_copy(meta_in, meta.at[mo, 0], load_sem.at[2]),
    ]
    w_ins = (wd_in, wg_in, wu_in)
    w_loads = [
        pltpu.make_async_copy(w_ins[k].at[0], w.at[k, own_rows], load_sem.at[3 + k])
        for k in range(3)
    ]
    for c in loads + w_loads:
        c.start()

    barrier = pltpu.get_barrier_semaphore()
    for d in range(1, inner):
        pl.semaphore_signal(barrier, inc=1, device_id={"expert": pal[d]}, device_id_type=mesh_id)
    pl.semaphore_signal(barrier, inc=1, device_id={"dp": other}, device_id_type=mesh_id)

    @pl.when(has_up)
    def _():
        pl.semaphore_signal(barrier, inc=1, device_id={"expert": me + inner}, device_id_type=mesh_id)

    @pl.when(has_dn)
    def _():
        pl.semaphore_signal(barrier, inc=1, device_id={"expert": me - inner}, device_id_type=mesh_id)

    pl.semaphore_wait(
        barrier, inner + has_up.astype(jnp.int32) + has_dn.astype(jnp.int32)
    )

    for c in loads:
        c.wait()

    def z_copy(kind, way, r):
        b = mo - r if way == 0 else mo + r
        to = me + inner if way == 0 else me - inner
        if kind == 2:
            return remote(meta.at[b, 0], meta.at[b, 0], ms_send.at[way, r], ms_recv.at[way, r], {"expert": to})
        return remote(
            col.at[kind, b], col.at[kind, b], z_send.at[kind, way, r], z_recv.at[kind, way, r], {"expert": to}
        )

    def sends_z(way, r):
        if way == 0:
            return jnp.logical_and(mo >= r, has_up)
        return jnp.logical_and(mo + r < outer, has_dn)

    def gets_z(way, r):
        return mo >= r + 1 if way == 0 else mo + r + 1 < outer

    def z_wait(kind, way, r):
        b = mo - 1 - r if way == 0 else mo + 1 + r
        frm = me - inner if way == 0 else me + inner
        if kind == 2:
            remote(meta.at[b, 0], meta.at[b, 0], ms_send.at[way, r], ms_recv.at[way, r], {"expert": frm}).wait_recv()
        else:
            remote(
                col.at[kind, b], col.at[kind, b], z_send.at[kind, way, r], z_recv.at[kind, way, r], {"expert": frm}
            ).wait_recv()

    def z_issue_tok(way, r):
        @pl.when(sends_z(way, r))
        def _():
            z_copy(2, way, r).start()
            z_copy(0, way, r).start()
            last = mo == r if way == 0 else mo + r == outer - 1

            @pl.when(last)
            def _():
                z_copy(1, way, 0).start()

    for way in (0, 1):
        z_issue_tok(way, 0)

    def w_copy(k):
        return remote(w_ins[k].at[0], w.at[k, own_rows], w_send.at[k], w_recv.at[k], {"dp": other})

    for k in (1, 2, 0):
        w_copy(k).start()

    sub = lax.broadcasted_iota(jnp.int32, (8, rows), 0)
    wanted = jnp.full((8, rows), -7, jnp.int32)
    for d in range(inner):
        wanted = jnp.where(sub == d, pal[d], wanted)
    near[...] = wanted.astype(F32)

    def earlier():
        a = lax.broadcasted_iota(jnp.int32, (rows, rows), 0)
        b = lax.broadcasted_iota(jnp.int32, (rows, rows), 1)
        return jnp.where(a < b, 1.0, 0.0).astype(BF16)

    def build(b):
        ids = meta[b, 0, 0:8, :]
        named = jnp.zeros((8, rows), F32)
        for k in range(top):
            named = named + jnp.where(ids[k:k + 1, :] == near[...], 1.0, 0.0)
        rank = dot(named.astype(BF16), earlier())
        spot = jnp.where(named > 0.0, rank, float(slot))
        within = lax.broadcasted_iota(jnp.int32, (slot, rows), 0).astype(F32)
        for d in range(inner):
            sel[b, d * slot:(d + 1) * slot, :] = jnp.where(spot[d:d + 1, :] == within, 1.0, 0.0).astype(BF16)

    def m_copy(b, d):
        return remote(meta.at[b, 0], meta.at[b, d], m_send.at[b, d], m_recv.at[b, d], {"expert": pal[d]})

    def p_copy(kind, b, d):
        part = pl.ds(d * slot, slot)
        dst = recv.at[kind, b, part] if kind < 2 else back.at[b, part]
        src = send.at[kind, b, part] if kind < 2 else send.at[0, b, part]
        return remote(src, dst, p_send.at[kind, b, d], p_recv.at[kind, b, d], {"expert": pal[d]})

    def scatter(kind, b):
        picked = dot(sel[b], col[kind, b]).astype(BF16)
        send[kind, b, slot:, :] = picked[slot:, :]
        recv[kind, b, :slot, :] = picked[:slot, :]
        for d in range(1, inner):
            p_copy(kind, b, d).start()

    def spread_tok(b):
        for d in range(1, inner):
            m_copy(b, d).start()
        build(b)
        scatter(0, b)

    spread_tok(mo)
    scatter(1, mo)
    for r in range(outer - 1):
        for way in (0, 1):
            @pl.when(gets_z(way, r))
            def _():
                z_wait(2, way, r)
                z_wait(0, way, r)
                if r + 1 < outer - 1:
                    z_issue_tok(way, r + 1)
        for way in (0, 1):
            @pl.when(gets_z(way, r))
            def _():
                spread_tok(mo - 1 - r if way == 0 else mo + 1 + r)

    def cot_round(r):
        for way in (0, 1):
            @pl.when(gets_z(way, r))
            def _():
                z_wait(1, way, r)
                if r + 1 < outer - 1:
                    @pl.when(sends_z(way, r + 1))
                    def _():
                        z_copy(1, way, r + 1).start()
        for way in (0, 1):
            @pl.when(gets_z(way, r))
            def _():
                scatter(1, mo - 1 - r if way == 0 else mo + 1 + r)

    for b in range(outer):
        for d in range(1, inner):
            m_copy(b, d).wait_recv()
    mine = jnp.full((8, rows), me, jnp.int32).astype(F32)
    for b in range(outer):
        for d in range(inner):
            q = b * inner + d
            same = meta[b, d, 0:8, :] == mine
            mask[q:q + 1, :] = jnp.sum(jnp.where(same, 1.0, 0.0), axis=0, keepdims=True)
            gq[q:q + 1, :] = jnp.sum(jnp.where(same, meta[b, d, 8:16, :], 0.0), axis=0, keepdims=True)
    held = mask[...].astype(BF16)
    ones = jnp.ones((rows, rows), BF16)
    begin = dot(dot(order_in[...], held).astype(BF16), ones)
    start[...] = begin
    count[...] = dot(held, ones)
    place[...] = jnp.where(mask[...] > 0.0, begin + dot(held, earlier()), float(CAP))
    within = lax.broadcasted_iota(jnp.int32, (slot, 128), 0).astype(F32)
    lane = lax.broadcasted_iota(jnp.int32, (slot, 128), 1).astype(F32)
    for q in range(size):
        target = jnp.where(within < count[q:q + 1, :128], start[q:q + 1, :128] + within, float(CAP))
        for j in range(CAP // 128):
            pack[q * slot:(q + 1) * slot, j * 128:(j + 1) * 128] = jnp.where(
                target == lane + float(j * 128), 1.0, 0.0
            ).astype(BF16)
    down = lax.broadcasted_iota(jnp.int32, (128, rows), 0).astype(F32)
    for j in range(CAP // 128):
        acc = jnp.zeros((128, rows), F32)
        for q in range(size):
            acc = acc + jnp.where(place[q:q + 1, :] == down + float(j * 128), gq[q:q + 1, :], 0.0)
        row_gate[j * 128:(j + 1) * 128, :] = jnp.broadcast_to(jnp.sum(acc, axis=1, keepdims=True), (128, 128))

    for b in range(outer):
        for d in range(1, inner):
            p_copy(0, b, d).wait_recv()

    def gather(kind, n):
        return dot_tn(pack[...], recv[kind, :, :, n].reshape(outer * span, n.size))

    def pack_x(n):
        x[:, n] = gather(0, n).astype(BF16)

    tiles(pack_x)
    cot_round(0)

    for k in (1, 2):
        w_loads[k].wait()
        w_copy(k).wait_recv()

    def forward(n):
        pre_gate = dot(x[...], w[1, :, n])
        pre_up = dot(x[...], w[2, :, n]) + 1.0
        sig = jax.nn.sigmoid(SWISH_SLOPE * pre_gate)
        value = pre_gate * sig
        slope = sig + SWISH_SLOPE * value * (1.0 - sig)
        act[:, n] = (value * pre_up).astype(BF16)
        coef[0, :, n] = pre_up * slope
        coef[1, :, n] = value

    tiles(forward)
    if outer > 2:
        cot_round(1)

    w_loads[0].wait()
    w_copy(0).wait_recv()

    def project(n):
        out[:, n] = (dot_nt(act[...], w[0, n, :]) * row_gate[:, :1]).astype(BF16)

    tiles(project)
    for r in range(2, outer - 1):
        cot_round(r)

    for b in range(outer):
        for d in range(1, inner):
            p_copy(0, b, d).wait_send()

    def give_back(b):
        part = pl.ds(pl.multiple_of(b * span, 16), span)
        rows_back = dot(pack[part, :], out[...]).astype(BF16)
        send[0, b, slot:, :] = rows_back[slot:, :]
        back[b, :slot, :] = rows_back[:slot, :]
        for d in range(1, inner):
            p_copy(2, b, d).start()

    for r in range(outer - 1, -1, -1):
        @pl.when(mo >= r)
        def _():
            give_back(mo - r)

        if r > 0:
            @pl.when(mo + r < outer)
            def _():
                give_back(mo + r)

    def flip_x(n):
        xt[1, n, :] = dot_tn(x[:, n], unit()).astype(BF16)

    def unit():
        a = lax.broadcasted_iota(jnp.int32, (CAP, CAP), 0)
        b = lax.broadcasted_iota(jnp.int32, (CAP, CAP), 1)
        return jnp.where(a == b, 1.0, 0.0).astype(BF16)

    tiles(flip_x)

    for b in range(outer):
        for d in range(1, inner):
            p_copy(1, b, d).wait_recv()

    def pack_g(n):
        g[:, n] = (gather(1, n) * row_gate[:, :1]).astype(BF16)

    tiles(pack_g)

    def flip_g(n):
        xt[0, n, :] = dot_tn(g[:, n], unit()).astype(BF16)

    tiles(flip_g)

    def back_act(n):
        d_hidden = dot(g[...], w[0, :, n])
        dact[0, :, n] = (d_hidden * coef[0, :, n]).astype(BF16)
        dact[1, :, n] = (d_hidden * coef[1, :, n]).astype(BF16)

    tiles(back_act)
    pl.semaphore_signal(free_sem, inc=1, device_id={"dp": other}, device_id_type=mesh_id)

    def r_copy(way, r):
        to = me - inner if way == 0 else me + inner
        return remote(
            zout.at[way, r - 1], zin.at[way, r - 1], r_send.at[way, r - 1], r_recv.at[way, r - 1], {"expert": to}
        )

    def partial(b):
        for d in range(1, inner):
            p_copy(2, b, d).wait_recv()
        return dot_tn(sel[b], back[b])

    def ret_round(r):
        for way in (0, 1):
            b = mo - r if way == 0 else mo + r
            inbound = has_up if way == 0 else has_dn
            if way == 1:
                inbound = mo > 0

            @pl.when(mo >= r if way == 0 else mo + r < outer)
            def _():
                zout[way, r - 1] = partial(b).astype(BF16)
                if r < outer - 1:
                    @pl.when(inbound)
                    def _():
                        r_copy(way, r + 1).wait_recv()
                        zout[way, r - 1] = (
                            zout[way, r - 1].astype(F32) + zin[way, r].astype(F32)
                        ).astype(BF16)
                r_copy(way, r).start()

    def ret_last():
        mixed_out[...] = partial(mo).astype(BF16)
        for way in (0, 1):
            @pl.when(has_up if way == 0 else has_dn)
            def _():
                r_copy(way, 1).wait_recv()
                mixed_out[...] = (mixed_out[...].astype(F32) + zin[way, 0].astype(F32)).astype(BF16)

    send_rows = pl.ds(0, shard)
    recv_rows = pl.ds(shard, shard)

    def g_copy(k):
        return remote(
            w.at[k, send_rows], w.at[k, recv_rows], g_send.at[k], g_recv.at[k], {"dp": other}
        )

    def right(k, n):
        return act[:, n] if k == 0 else dact[k - 1, :, n]

    their_rows = pl.ds(pl.multiple_of(other * shard, 16), shard)
    for r in range(outer - 1, 1, -1):
        ret_round(r)
    for k in range(3):
        lhs = 0 if k == 0 else 1

        def theirs(n):
            w[k, send_rows, n] = dot(xt[lhs, their_rows, :], right(k, n)).astype(BF16)

        tiles(theirs)
        if k == 0:
            pl.semaphore_wait(free_sem, 1)
        g_copy(k).start()
        if k == 0 and outer > 1:
            ret_round(1)
    ret_last()
    outs = (gd_out, gg_out, gu_out)
    stores = []
    for k in range(3):
        lhs = 0 if k == 0 else 1
        g_copy(k).wait_recv()

        def ours(n):
            total = dot(xt[lhs, own_rows, :], right(k, n)) + w[k, recv_rows, n].astype(F32)
            w[k, recv_rows, n] = total.astype(BF16)

        tiles(ours)
        store = pltpu.make_async_copy(w.at[k, recv_rows], outs[k].at[0], o_sem.at[k])
        store.start()
        stores.append(store)

    for way in (0, 1):
        for r in range(outer - 1):
            @pl.when(sends_z(way, r))
            def _():
                for kind in (0, 1, 2):
                    z_copy(kind, way, r).wait_send()
        for r in range(1, outer):
            @pl.when(mo >= r if way == 0 else mo + r < outer)
            def _():
                r_copy(way, r).wait_send()
    for b in range(outer):
        for d in range(1, inner):
            m_copy(b, d).wait_send()
            p_copy(1, b, d).wait_send()
            p_copy(2, b, d).wait_send()
    for k in range(3):
        w_copy(k).wait_send()
        g_copy(k).wait_send()
        stores[k].wait()


def fits(args):
    rows = args[0].shape[0]
    shard = args[4].shape[1]
    size = lax.axis_size("expert")
    return (
        lax.axis_size("dp") == 2 and shard % 16 == 0 and rows == 128
        and size % INNER == 0 and INNER < size <= 16
    )


def fused_layer(tokens, cotangent, expert_ids, gate_weights, w_gate, w_up, w_down):
    size = lax.axis_size("expert")
    rows, top = expert_ids.shape
    width = tokens.shape[1]
    shard = w_gate.shape[1]
    hid = w_gate.shape[2]
    inner = INNER
    outer = size // inner
    slot = -(-3 * rows * top // (2 * size) // 16) * 16
    span = inner * slot
    me = lax.axis_index("expert")
    meta = jnp.concatenate([
        jnp.pad(expert_ids.T.astype(F32), ((0, 8 - top), (0, 0)), constant_values=-1.0),
        jnp.pad(gate_weights.T, ((0, 8 - top), (0, 0))),
    ], axis=0)
    which = jnp.arange(size, dtype=jnp.int32)
    source = which // inner * inner + jnp.bitwise_xor(me % inner, which % inner)
    order = (source[None, :] < source[:, None]).astype(BF16)
    dims = (size, outer, inner, rows, width, top, slot, shard)
    anywhere = pl.BlockSpec(memory_space=pl.ANY)
    vmem = pl.BlockSpec(memory_space=pltpu.VMEM)
    dma = pltpu.SemaphoreType.DMA
    hop = outer - 1
    scratch = [
        pltpu.VMEM((2, outer, rows, width), BF16),
        pltpu.VMEM((outer, inner, 16, rows), F32),
        pltpu.VMEM((outer, span, rows), BF16),
        pltpu.VMEM((2, outer, span, width), BF16),
        pltpu.VMEM((2, outer, span, width), BF16),
        pltpu.VMEM((outer, span, width), BF16),
        pltpu.VMEM((outer * span, CAP), BF16),
        pltpu.VMEM((CAP, width), BF16),
        pltpu.VMEM((CAP, hid), BF16),
        pltpu.VMEM((CAP, width), BF16),
        pltpu.VMEM((CAP, width), BF16),
        pltpu.VMEM((2, CAP, hid), F32),
        pltpu.VMEM((3, 2 * shard, hid), BF16),
        pltpu.VMEM((2, width, CAP), BF16),
        pltpu.VMEM((2, CAP, hid), BF16),
        pltpu.VMEM((2, hop, rows, width), BF16),
        pltpu.VMEM((2, hop, rows, width), BF16),
        pltpu.VMEM((8, rows), F32),
        pltpu.VMEM((size, rows), F32),
        pltpu.VMEM((size, rows), F32),
        pltpu.VMEM((size, rows), F32),
        pltpu.VMEM((size, rows), F32),
        pltpu.VMEM((size, rows), F32),
        pltpu.VMEM((CAP, 128), F32),
        dma((6,)), dma((2, 2, hop)), dma((2, 2, hop)),
        dma((outer, inner)), dma((outer, inner)), dma((2, hop)), dma((2, hop)),
        dma((3, outer, inner)), dma((3, outer, inner)),
        dma((3,)), dma((3,)), dma((2, hop)), dma((2, hop)), dma((3,)), dma((3,)), dma((3,)),
        pltpu.SemaphoreType.REGULAR,
    ]
    grad = jax.ShapeDtypeStruct(w_gate.shape, BF16)
    mixed, gd, gg, gu = pl.pallas_call(
        functools.partial(step_kernel, dims),
        out_shape=(jax.ShapeDtypeStruct((rows, width), BF16), grad, grad, grad),
        in_specs=[anywhere, anywhere, anywhere, vmem, anywhere, anywhere, anywhere],
        out_specs=(vmem, anywhere, anywhere, anywhere),
        scratch_shapes=scratch,
        compiler_params=pltpu.CompilerParams(
            collective_id=1, has_side_effects=True, vmem_limit_bytes=67043328
        ),
    )(tokens, cotangent, meta, order, w_gate, w_up, w_down)
    return mixed, gg, gu, gd


def body(*args):
    if fits(args):
        return fused_layer(*args)
    return layer(*args)


def solution(mesh):
    rows = P(("expert", "dp"), None)
    mats = P("expert", "dp", None)
    return jax.shard_map(
        body,
        mesh=mesh,
        in_specs=(rows, rows, rows, rows, mats, mats, mats),
        out_specs=(rows, mats, mats, mats),
        check_vma=False,
    )
```

```python
import functools

import jax
import jax.numpy as jnp
from jax import lax
from jax.experimental import pallas as pl
from jax.experimental.pallas import tpu as pltpu
from jax.sharding import PartitionSpec as P


CAP = 512
INNER = 4
TILE = 512
PIECES = 2
SWISH_SLOPE = 1.702
F32 = jnp.float32
BF16 = jnp.bfloat16


def dot(a, b):
    return jnp.dot(a, b, preferred_element_type=F32)


def dot_nt(a, b):
    return lax.dot_general(a, b, (((1,), (1,)), ((), ())), preferred_element_type=F32)


def dot_tn(a, b):
    return lax.dot_general(a, b, (((0,), (0,)), ((), ())), preferred_element_type=F32)


def share_kernel(size, x_ref, all_ref, send_sem, recv_sem):
    me = lax.axis_index("expert")
    barrier = pltpu.get_barrier_semaphore()
    for k in range(1, size):
        pl.semaphore_signal(
            barrier, inc=1, device_id={"expert": lax.rem(me + k, size)},
            device_id_type=pl.DeviceIdType.MESH,
        )
    pl.semaphore_wait(barrier, size - 1)
    copies = []
    for k in range(1, size):
        copy = pltpu.make_async_remote_copy(
            src_ref=x_ref, dst_ref=all_ref.at[me],
            send_sem=send_sem.at[k], recv_sem=recv_sem.at[k],
            device_id={"expert": lax.rem(me + k, size)},
            device_id_type=pl.DeviceIdType.MESH,
        )
        copy.start()
        copies.append(copy)
    all_ref[me] = x_ref[...]
    for copy in copies:
        copy.wait()


def share(x):
    size = lax.axis_size("expert")
    return pl.pallas_call(
        functools.partial(share_kernel, size),
        out_shape=jax.ShapeDtypeStruct((size,) + x.shape, x.dtype),
        in_specs=[pl.BlockSpec(memory_space=pltpu.VMEM)],
        out_specs=pl.BlockSpec(memory_space=pltpu.VMEM),
        scratch_shapes=[
            pltpu.SemaphoreType.DMA((size,)),
            pltpu.SemaphoreType.DMA((size,)),
        ],
        compiler_params=pltpu.CompilerParams(collective_id=0, has_side_effects=True),
    )(x)


def layer(tokens, cotangent, expert_ids, gate_weights, w_gate, w_up, w_down):
    size = lax.axis_size("expert")
    rows, top = expert_ids.shape
    width = tokens.shape[1]
    slot = 3 * rows * top // (2 * size)
    inner = min(INNER, size)
    outer = size // inner
    me = lax.axis_index("expert")
    mine_out, mine_in = me // inner, me % inner
    half = outer // 2
    partner = jnp.bitwise_xor(mine_in, jnp.arange(inner, dtype=jnp.int32))

    def shift(x, by):
        pairs = [(d, (d // inner + by) % outer * inner + d % inner) for d in range(size)]
        return lax.ppermute(x, "expert", pairs)

    def gather_outer(x):
        blocks = [x] + [None] * (outer - 1)
        for r in range(1, half + 1):
            if outer > 1:
                blocks[r] = shift(blocks[r - 1], 1)
        for r in range(1, outer - half):
            blocks[outer - r] = shift(blocks[(outer - r + 1) % outer], -1)
        return blocks

    def exchange(blocks):
        moved = list(blocks)
        for d in range(inner - 1, 0, -1):
            pairs = [(e, e // inner * inner + (e % inner ^ d)) for e in range(size)]
            moved[d] = lax.ppermute(blocks[d], "expert", pairs)
        return jnp.concatenate(moved)

    def relay(blocks):
        held = jnp.concatenate(blocks)
        return exchange([dot(part, held).astype(BF16) for part in select])

    meta = jnp.concatenate([expert_ids.T.astype(F32), gate_weights.T], axis=0)
    meta_all = share(meta)
    meta_all, tokens = lax.optimization_barrier((meta_all, tokens))
    token_blocks = gather_outer(tokens)
    token_blocks, cotangent = lax.optimization_barrier((token_blocks, cotangent))
    cot_blocks = gather_outer(cotangent)

    ids_all = meta_all[:, :top, :].astype(jnp.int32)
    gates_all = meta_all[:, top:, :]
    back = (mine_out - jnp.arange(outer, dtype=jnp.int32)) % outer

    before = (jnp.arange(rows)[:, None] < jnp.arange(rows)[None, :]).astype(BF16)

    ids_relay = jnp.stack([
        lax.dynamic_index_in_dim(ids_all, back[r] * inner + mine_in, 0, keepdims=False)
        for r in range(outer)
    ])
    near = mine_out * inner + partner
    named = jnp.any(ids_relay[None] == near[:, None, None, None], axis=2)
    rank = dot(named.astype(BF16).reshape(inner * outer, rows), before)
    rank = rank.reshape(inner, outer, rows).astype(jnp.int32)
    place = jnp.where(named, rank, slot)
    hit = place[:, :, None, :] == jnp.arange(slot, dtype=jnp.int32)[None, None, :, None]
    same = jnp.eye(outer, dtype=jnp.bool_)
    select = (hit[:, :, :, None, :] & same[None, :, None, :, None]).astype(BF16)
    select = select.reshape(inner, outer * slot, outer * rows)

    mask = jnp.any(ids_all == me, axis=1)
    gate_of = jnp.sum(jnp.where(ids_all == me, gates_all, 0.0), axis=1)
    counts = jnp.sum(mask.astype(jnp.int32), axis=1)
    below = jnp.arange(size)[:, None] > jnp.arange(size)[None, :]
    starts = jnp.sum(jnp.where(below, counts[None, :], 0), axis=1)
    own_rank = dot(mask.astype(BF16), before).astype(jnp.int32)
    position = jnp.where(mask, starts[:, None] + own_rank, CAP).reshape(1, size * rows)
    row_index = jnp.arange(CAP, dtype=jnp.int32)
    row_gate = jnp.sum(
        jnp.where(position == row_index[:, None], gate_of.reshape(1, size * rows), 0.0),
        axis=1, keepdims=True,
    )
    source = back[None, :] * inner + partner[:, None]
    is_source = source[:, :, None] == jnp.arange(size, dtype=jnp.int32)
    slot_start = jnp.sum(jnp.where(is_source, starts, 0), axis=2)
    slot_live = jnp.sum(jnp.where(is_source, counts, 0), axis=2)
    within = jnp.arange(slot, dtype=jnp.int32)
    slot_row = jnp.where(
        within < slot_live[:, :, None], slot_start[:, :, None] + within, CAP
    ).reshape(1, inner * outer * slot)
    pack = (row_index[:, None] == slot_row).astype(BF16)

    full_gate, full_up, full_down = (
        lax.all_gather(w_gate, "dp", axis=1, tiled=True)[0],
        lax.all_gather(w_up, "dp", axis=1, tiled=True)[0],
        lax.all_gather(w_down, "dp", axis=1, tiled=True)[0],
    )

    recv_x = relay(token_blocks)
    packed_x = dot(pack, recv_x).astype(BF16)
    pre_gate = dot(packed_x, full_gate)
    pre_up = dot(packed_x, full_up)
    sig = jax.nn.sigmoid(SWISH_SLOPE * pre_gate)
    value = pre_gate * sig
    slope = sig + SWISH_SLOPE * pre_gate * sig * (1.0 - sig)
    hidden = (value * (pre_up + 1.0)).astype(BF16)
    out = (dot_nt(hidden, full_down) * row_gate).astype(BF16)
    spread = dot_tn(pack, out).astype(BF16).reshape(inner, outer * slot, width)

    recv_g = relay(cot_blocks)
    spread, recv_g = lax.optimization_barrier((spread, recv_g))
    returned = exchange([spread[d] for d in range(inner)])
    packed_g = (dot(pack, recv_g) * row_gate).astype(BF16)
    grad_down = dot_tn(packed_g, hidden).astype(BF16)
    d_hidden = dot(packed_g, full_down)
    d_gate = (d_hidden * (pre_up + 1.0) * slope).astype(BF16)
    d_up = (d_hidden * value).astype(BF16)
    returned, d_gate, d_up = lax.optimization_barrier((returned, d_gate, d_up))
    partial = dot_tn(select.reshape(inner * outer * slot, outer * rows), returned)
    partial = partial.reshape(outer, rows, width)
    partial, d_gate, d_up = lax.optimization_barrier((partial, d_gate, d_up))
    grad_gate = dot_tn(packed_x, d_gate).astype(BF16)
    grad_up = dot_tn(packed_x, d_up).astype(BF16)

    total = partial[0]
    ahead = partial[half]
    behind = partial[half + 1] if outer - half > 1 else None
    for r in range(half - 1, -1, -1):
        ahead = shift(ahead.astype(BF16), -1).astype(F32)
        if r > 0:
            ahead = ahead + partial[r]
    for r in range(half + 2, outer + 1):
        behind = shift(behind.astype(BF16), 1).astype(F32)
        if r < outer:
            behind = behind + partial[r]
    if half > 0:
        total = total + ahead
    if behind is not None:
        total = total + behind
    mixed = total.astype(BF16)

    grads = [
        lax.psum_scatter(g, "dp", scatter_dimension=0, tiled=True)[None]
        for g in (grad_down, grad_gate, grad_up)
    ]
    return mixed, grads[1], grads[2], grads[0]


def flip(i, d):
    out, bit = 0, 1
    while bit <= max(d, INNER - 1):
        out = out + lax.rem(lax.rem(i // bit, 2) + (d // bit) % 2, 2) * bit
        bit *= 2
    return out


def step_kernel(
    dims, tok_in, cot_in, ids_in, gates_in, wg_in, wu_in, wd_in,
    mixed_out, gd_out, gg_out, gu_out,
    ids_buf, gates_buf, col, meta, sel, send, recv, back, pack, x, act, out, g, coef, w, xt, dact,
    zin, zout, near, mask, gq, start, count, place, row_gate, total,
    load_sem, z_send, z_recv, m_send, m_recv, ms_send, ms_recv, p_send, p_recv,
    w_send, w_recv, r_send, r_recv, g_send, g_recv, free_sem,
):
    size, outer, inner, rows, width, top, slot, shard = dims
    span = inner * slot
    me = lax.axis_index("expert")
    dp = lax.axis_index("dp")
    mo, mi = me // inner, lax.rem(me, inner)
    pal = [flip(mi, d) + mo * inner for d in range(inner)]
    other = 1 - dp
    has_up, has_dn = mo < outer - 1, mo > 0
    mesh_id = pl.DeviceIdType.MESH

    def remote(src, dst, ss, rs, device):
        return pltpu.make_async_remote_copy(
            src_ref=src, dst_ref=dst, send_sem=ss, recv_sem=rs,
            device_id=device, device_id_type=mesh_id,
        )

    def tiles(fn):
        full = width // TILE
        if full:
            def step(i, carry):
                fn(pl.ds(pl.multiple_of(i * TILE, TILE), TILE))
                return carry

            lax.fori_loop(0, full, step, 0)
        if width % TILE:
            fn(pl.ds(full * TILE, width % TILE))

    def zero_ends():
        for way, has in ((0, has_up), (1, has_dn)):
            @pl.when(jnp.logical_not(has))
            def _():
                zin[way, 0] = jnp.zeros((width, rows), BF16)

    own_rows = pl.ds(pl.multiple_of(dp * shard, 16), shard)
    loads = [
        pltpu.make_async_copy(tok_in, col.at[0, mo], load_sem.at[0]),
        pltpu.make_async_copy(cot_in, col.at[1, mo], load_sem.at[1]),
        pltpu.make_async_copy(ids_in, ids_buf, load_sem.at[2]),
        pltpu.make_async_copy(gates_in, gates_buf, load_sem.at[6]),
    ]
    w_ins = (wd_in, wg_in, wu_in)
    w_loads = [
        pltpu.make_async_copy(w_ins[k].at[0], w.at[k, own_rows], load_sem.at[3 + k])
        for k in range(3)
    ]
    for c in loads + w_loads:
        c.start()

    barrier = pltpu.get_barrier_semaphore()
    for d in range(1, inner):
        pl.semaphore_signal(barrier, inc=1, device_id={"expert": pal[d]}, device_id_type=mesh_id)
    pl.semaphore_signal(barrier, inc=1, device_id={"dp": other}, device_id_type=mesh_id)

    @pl.when(has_up)
    def _():
        pl.semaphore_signal(barrier, inc=1, device_id={"expert": me + inner}, device_id_type=mesh_id)

    @pl.when(has_dn)
    def _():
        pl.semaphore_signal(barrier, inc=1, device_id={"expert": me - inner}, device_id_type=mesh_id)

    zero_ends()
    for c in loads[2:]:
        c.wait()
    meta[mo, 0, 0:8, :] = jnp.full((8, rows), -1.0, F32)
    meta[mo, 0, 8:16, :] = jnp.zeros((8, rows), F32)
    meta[mo, 0, 0:top, :] = ids_buf[...].astype(F32)
    meta[mo, 0, 8:8 + top, :] = gates_buf[...]
    for c in loads[:2]:
        c.wait()
    pl.semaphore_wait(
        barrier, inner + has_up.astype(jnp.int32) + has_dn.astype(jnp.int32)
    )


    def piece(h):
        return pl.ds(h * (width // PIECES), width // PIECES)

    def z_copy(kind, way, r, h=0):
        b = mo - r if way == 0 else mo + r
        to = me + inner if way == 0 else me - inner
        if kind == 2:
            return remote(meta.at[b, 0], meta.at[b, 0], ms_send.at[way, r], ms_recv.at[way, r], {"expert": to})
        part = col.at[kind, b, piece(h)]
        return remote(part, part, z_send.at[kind, way, r, h], z_recv.at[kind, way, r, h], {"expert": to})

    def sends_z(way, r):
        if way == 0:
            return jnp.logical_and(mo >= r, has_up)
        return jnp.logical_and(mo + r < outer, has_dn)

    def gets_z(way, r):
        return mo >= r + 1 if way == 0 else mo + r + 1 < outer

    def z_wait(kind, way, r, h=0):
        b = mo - 1 - r if way == 0 else mo + 1 + r
        frm = me - inner if way == 0 else me + inner
        if kind == 2:
            remote(meta.at[b, 0], meta.at[b, 0], ms_send.at[way, r], ms_recv.at[way, r], {"expert": frm}).wait_recv()
        else:
            part = col.at[kind, b, piece(h)]
            remote(
                part, part, z_send.at[kind, way, r, h], z_recv.at[kind, way, r, h], {"expert": frm}
            ).wait_recv()

    def z_issue(kind, way, r, h):
        @pl.when(sends_z(way, r))
        def _():
            if kind == 0 and h == 0:
                z_copy(2, way, r).start()
            z_copy(kind, way, r, h).start()
            if kind == 0 and h == PIECES - 1:
                last = mo == r if way == 0 else mo + r == outer - 1

                @pl.when(last)
                def _():
                    for i in range(PIECES):
                        z_copy(1, way, 0, i).start()

    def z_round(kind, r):
        for h in range(PIECES):
            for way in (0, 1):
                @pl.when(gets_z(way, r))
                def _():
                    if kind == 0 and h == 0:
                        z_wait(2, way, r)
                    z_wait(kind, way, r, h)
                    if r + 1 < outer - 1:
                        z_issue(kind, way, r + 1, h)

    for h in range(PIECES):
        for way in (0, 1):
            z_issue(0, way, 0, h)

    def w_copy(k):
        return remote(w_ins[k].at[0], w.at[k, own_rows], w_send.at[k], w_recv.at[k], {"dp": other})

    for k in (1, 2, 0):
        w_copy(k).start()

    sub = lax.broadcasted_iota(jnp.int32, (8, rows), 0)
    wanted = jnp.full((8, rows), -7, jnp.int32)
    for d in range(inner):
        wanted = jnp.where(sub == d, pal[d], wanted)
    near[...] = wanted.astype(F32)

    def earlier():
        a = lax.broadcasted_iota(jnp.int32, (rows, rows), 0)
        b = lax.broadcasted_iota(jnp.int32, (rows, rows), 1)
        return jnp.where(a < b, 1.0, 0.0).astype(BF16)

    def build(b):
        ids = meta[b, 0, 0:8, :]
        named = jnp.zeros((8, rows), F32)
        for k in range(top):
            named = named + jnp.where(ids[k:k + 1, :] == near[...], 1.0, 0.0)
        rank = dot(named.astype(BF16), earlier())
        spot = jnp.where(named > 0.0, rank, float(slot))
        within = lax.broadcasted_iota(jnp.int32, (slot, rows), 0).astype(F32)
        for d in range(inner):
            sel[b, d * slot:(d + 1) * slot, :] = jnp.where(spot[d:d + 1, :] == within, 1.0, 0.0).astype(BF16)

    def m_copy(b, d):
        return remote(meta.at[b, 0], meta.at[b, d], m_send.at[b, d], m_recv.at[b, d], {"expert": pal[d]})

    def p_copy(kind, b, d):
        part = pl.ds(d * slot, slot)
        dst = recv.at[kind, b, part] if kind < 2 else back.at[b, part]
        src = send.at[kind, b, part] if kind < 2 else send.at[0, b, part]
        return remote(src, dst, p_send.at[kind, b, d], p_recv.at[kind, b, d], {"expert": pal[d]})

    def scatter(kind, b):
        picked = dot_nt(sel[b], col[kind, b]).astype(BF16)
        send[kind, b, slot:, :] = picked[slot:, :]
        recv[kind, b, :slot, :] = picked[:slot, :]
        for d in range(1, inner):
            p_copy(kind, b, d).start()

    def spread_tok(b):
        for d in range(1, inner):
            m_copy(b, d).start()
        build(b)
        scatter(0, b)

    spread_tok(mo)
    scatter(1, mo)
    for r in range(outer - 1):
        z_round(0, r)
        for way in (0, 1):
            @pl.when(gets_z(way, r))
            def _():
                spread_tok(mo - 1 - r if way == 0 else mo + 1 + r)

    at_end = jnp.logical_or(mo == 0, mo == outer - 1)
    inside = jnp.logical_not(at_end)

    def cot_round(r):
        z_round(1, r)
        for way in (0, 1):
            @pl.when(gets_z(way, r))
            def _():
                scatter(1, mo - 1 - r if way == 0 else mo + 1 + r)

    def cot_at(r, when):
        if r < outer - 1:
            @pl.when(when)
            def _():
                cot_round(r)

    for b in range(outer):
        for d in range(1, inner):
            m_copy(b, d).wait_recv()
    mine = jnp.full((8, rows), me, jnp.int32).astype(F32)
    for b in range(outer):
        for d in range(inner):
            q = b * inner + d
            same = meta[b, d, 0:8, :] == mine
            mask[q:q + 1, :] = jnp.sum(jnp.where(same, 1.0, 0.0), axis=0, keepdims=True)
            gq[q:q + 1, :] = jnp.sum(jnp.where(same, meta[b, d, 8:16, :], 0.0), axis=0, keepdims=True)
    held = mask[...].astype(BF16)
    first = jnp.bitwise_xor(lax.broadcasted_iota(jnp.int32, (size, size), 0), mi)
    second = jnp.bitwise_xor(lax.broadcasted_iota(jnp.int32, (size, size), 1), mi)
    order = jnp.where(second < first, 1.0, 0.0).astype(BF16)
    ones = jnp.ones((rows, rows), BF16)
    begin = dot(dot(order, held).astype(BF16), ones)
    start[...] = begin
    count[...] = dot(held, ones)
    place[...] = jnp.where(mask[...] > 0.0, begin + dot(held, earlier()), float(CAP))
    within = lax.broadcasted_iota(jnp.int32, (slot, 128), 0).astype(F32)
    lane = lax.broadcasted_iota(jnp.int32, (slot, 128), 1).astype(F32)
    for q in range(size):
        target = jnp.where(within < count[q:q + 1, :128], start[q:q + 1, :128] + within, float(CAP))
        for j in range(CAP // 128):
            pack[q * slot:(q + 1) * slot, j * 128:(j + 1) * 128] = jnp.where(
                target == lane + float(j * 128), 1.0, 0.0
            ).astype(BF16)
    down = lax.broadcasted_iota(jnp.int32, (128, rows), 0).astype(F32)
    for j in range(CAP // 128):
        acc = jnp.zeros((128, rows), F32)
        for q in range(size):
            acc = acc + jnp.where(place[q:q + 1, :] == down + float(j * 128), gq[q:q + 1, :], 0.0)
        row_gate[j * 128:(j + 1) * 128, :] = jnp.broadcast_to(jnp.sum(acc, axis=1, keepdims=True), (128, 128))

    cot_at(0, inside)
    for b in range(outer):
        for d in range(1, inner):
            p_copy(0, b, d).wait_recv()

    def gather(kind, n):
        return dot_tn(pack[...], recv[kind, :, :, n].reshape(outer * span, n.size))

    def pack_x(n):
        x[:, n] = gather(0, n).astype(BF16)

    tiles(pack_x)
    cot_at(0, at_end)
    cot_at(1, inside)

    for k in (1, 2):
        w_loads[k].wait()
        w_copy(k).wait_recv()

    def forward(n):
        pre_gate = dot(x[...], w[1, :, n])
        pre_up = dot(x[...], w[2, :, n]) + 1.0
        sig = jax.nn.sigmoid(SWISH_SLOPE * pre_gate)
        value = pre_gate * sig
        slope = sig + SWISH_SLOPE * value * (1.0 - sig)
        act[:, n] = (value * pre_up).astype(BF16)
        coef[0, :, n] = pre_up * slope
        coef[1, :, n] = value

    tiles(forward)
    cot_at(1, at_end)

    w_loads[0].wait()
    w_copy(0).wait_recv()

    def project(n):
        out[:, n] = (dot_nt(act[...], w[0, n, :]) * row_gate[:, :1]).astype(BF16)

    tiles(project)

    for b in range(outer):
        for d in range(1, inner):
            p_copy(0, b, d).wait_send()

    def give_back(b):
        part = pl.ds(pl.multiple_of(b * span, 16), span)
        rows_back = dot(pack[part, :], out[...]).astype(BF16)
        send[0, b, slot:, :] = rows_back[slot:, :]
        back[b, :slot, :] = rows_back[:slot, :]
        for d in range(1, inner):
            p_copy(2, b, d).start()

    def give_round(r):
        @pl.when(mo >= r)
        def _():
            give_back(mo - r)

        if r > 0:
            @pl.when(mo + r < outer)
            def _():
                give_back(mo + r)

    give_round(outer - 1)
    for r in range(2, outer - 1):
        cot_round(r)
    for r in range(outer - 2, -1, -1):
        give_round(r)

    def r_copy(way, r, h):
        to = me - inner if way == 0 else me + inner
        return remote(
            zout.at[way, r - 1, piece(h)], zin.at[way, r - 1, piece(h)],
            r_send.at[way, r - 1, h], r_recv.at[way, r - 1, h], {"expert": to},
        )

    def partial(b):
        for d in range(1, inner):
            p_copy(2, b, d).wait_recv()
        return dot_tn(back[b], sel[b])

    def gives(way, r):
        return mo >= r if way == 0 else mo + r < outer

    def ret_round(r):
        for way in (0, 1):
            @pl.when(gives(way, r))
            def _():
                zout[way, r - 1] = partial(mo - r if way == 0 else mo + r).astype(BF16)
        for h in range(PIECES):
            for way, inbound in ((0, has_up), (1, has_dn)):
                @pl.when(gives(way, r))
                def _():
                    if r < outer - 1:
                        @pl.when(inbound)
                        def _():
                            r_copy(way, r + 1, h).wait_recv()
                            zout[way, r - 1, piece(h)] = (
                                zout[way, r - 1, piece(h)].astype(F32) + zin[way, r, piece(h)].astype(F32)
                            ).astype(BF16)
                    r_copy(way, r, h).start()

    def ret_last():
        total[...] = partial(mo)
        for h in range(PIECES):
            for way, inbound in ((0, has_up), (1, has_dn)):
                @pl.when(inbound)
                def _():
                    r_copy(way, 1, h).wait_recv()
            mixed_out[piece(h)] = (
                total[piece(h)] + zin[0, 0, piece(h)].astype(F32) + zin[1, 0, piece(h)].astype(F32)
            ).astype(BF16)

    def flip_x(n):
        xt[1, n, :] = dot_tn(x[:, n], unit()).astype(BF16)

    def unit():
        a = lax.broadcasted_iota(jnp.int32, (CAP, CAP), 0)
        b = lax.broadcasted_iota(jnp.int32, (CAP, CAP), 1)
        return jnp.where(a == b, 1.0, 0.0).astype(BF16)

    tiles(flip_x)
    ret_round(outer - 1)

    for b in range(outer):
        for d in range(1, inner):
            p_copy(1, b, d).wait_recv()

    def pack_g(n):
        g[:, n] = (gather(1, n) * row_gate[:, :1]).astype(BF16)

    tiles(pack_g)

    def flip_g(n):
        xt[0, n, :] = dot_tn(g[:, n], unit()).astype(BF16)

    tiles(flip_g)

    def back_act(n):
        d_hidden = dot(g[...], w[0, :, n])
        dact[0, :, n] = (d_hidden * coef[0, :, n]).astype(BF16)
        dact[1, :, n] = (d_hidden * coef[1, :, n]).astype(BF16)

    tiles(back_act)
    pl.semaphore_signal(free_sem, inc=1, device_id={"dp": other}, device_id_type=mesh_id)

    send_rows = pl.ds(0, shard)
    recv_rows = pl.ds(shard, shard)

    def g_copy(k):
        return remote(
            w.at[k, send_rows], w.at[k, recv_rows], g_send.at[k], g_recv.at[k], {"dp": other}
        )

    def right(k, n):
        return act[:, n] if k == 0 else dact[k - 1, :, n]

    their_rows = pl.ds(pl.multiple_of(other * shard, 16), shard)
    for r in range(outer - 2, 1, -1):
        ret_round(r)
    for k in range(3):
        lhs = 0 if k == 0 else 1

        def theirs(n):
            w[k, send_rows, n] = dot(xt[lhs, their_rows, :], right(k, n)).astype(BF16)

        tiles(theirs)
        if k == 0:
            pl.semaphore_wait(free_sem, 1)
        g_copy(k).start()
    if outer > 2:
        ret_round(1)
    outs = (gd_out, gg_out, gu_out)
    for k in range(3):
        lhs = 0 if k == 0 else 1
        g_copy(k).wait_recv()

        def ours(n):
            grad = dot(xt[lhs, own_rows, :], right(k, n)) + w[k, recv_rows, n].astype(F32)
            outs[k][0, :, n] = grad.astype(BF16)

        tiles(ours)

    ret_last()

    for way in (0, 1):
        for r in range(outer - 1):
            @pl.when(sends_z(way, r))
            def _():
                z_copy(2, way, r).wait_send()
                for h in range(PIECES):
                    z_copy(0, way, r, h).wait_send()
                    z_copy(1, way, r, h).wait_send()
        for r in range(1, outer):
            @pl.when(mo >= r if way == 0 else mo + r < outer)
            def _():
                for h in range(PIECES):
                    r_copy(way, r, h).wait_send()
    for b in range(outer):
        for d in range(1, inner):
            m_copy(b, d).wait_send()
            p_copy(1, b, d).wait_send()
            p_copy(2, b, d).wait_send()
    for k in range(3):
        w_copy(k).wait_send()
        g_copy(k).wait_send()


def store_kernel(*refs):
    sem = refs[-1]
    copies = [pltpu.make_async_copy(refs[k], refs[4 + k], sem.at[k]) for k in range(4)]
    for c in copies:
        c.start()
    for c in copies:
        c.wait()


def fits(args):
    rows = args[0].shape[0]
    shard = args[4].shape[1]
    size = lax.axis_size("expert")
    return (
        lax.axis_size("dp") == 2 and shard % 16 == 0 and rows == 128
        and size % INNER == 0 and INNER < size <= 16
    )


def fused_layer(tokens, cotangent, expert_ids, gate_weights, w_gate, w_up, w_down):
    size = lax.axis_size("expert")
    rows, top = expert_ids.shape
    width = tokens.shape[1]
    shard = w_gate.shape[1]
    hid = w_gate.shape[2]
    inner = INNER
    outer = size // inner
    slot = -(-3 * rows * top // (2 * size) // 16) * 16
    span = inner * slot
    dims = (size, outer, inner, rows, width, top, slot, shard)
    anywhere = pl.BlockSpec(memory_space=pl.ANY)
    dma = pltpu.SemaphoreType.DMA
    hop = outer - 1
    scratch = [
        pltpu.VMEM((top, rows), jnp.int32),
        pltpu.VMEM((top, rows), F32),
        pltpu.VMEM((2, outer, width, rows), BF16),
        pltpu.VMEM((outer, inner, 16, rows), F32),
        pltpu.VMEM((outer, span, rows), BF16),
        pltpu.VMEM((2, outer, span, width), BF16),
        pltpu.VMEM((2, outer, span, width), BF16),
        pltpu.VMEM((outer, span, width), BF16),
        pltpu.VMEM((outer * span, CAP), BF16),
        pltpu.VMEM((CAP, width), BF16),
        pltpu.VMEM((CAP, hid), BF16),
        pltpu.VMEM((CAP, width), BF16),
        pltpu.VMEM((CAP, width), BF16),
        pltpu.VMEM((2, CAP, hid), F32),
        pltpu.VMEM((3, 2 * shard, hid), BF16),
        pltpu.VMEM((2, width, CAP), BF16),
        pltpu.VMEM((2, CAP, hid), BF16),
        pltpu.VMEM((2, hop, width, rows), BF16),
        pltpu.VMEM((2, hop, width, rows), BF16),
        pltpu.VMEM((8, rows), F32),
        pltpu.VMEM((size, rows), F32),
        pltpu.VMEM((size, rows), F32),
        pltpu.VMEM((size, rows), F32),
        pltpu.VMEM((size, rows), F32),
        pltpu.VMEM((size, rows), F32),
        pltpu.VMEM((CAP, 128), F32),
        pltpu.VMEM((width, rows), F32),
        dma((7,)), dma((2, 2, hop, PIECES)), dma((2, 2, hop, PIECES)),
        dma((outer, inner)), dma((outer, inner)), dma((2, hop)), dma((2, hop)),
        dma((3, outer, inner)), dma((3, outer, inner)),
        dma((3,)), dma((3,)), dma((2, hop, PIECES)), dma((2, hop, PIECES)), dma((3,)), dma((3,)),
        pltpu.SemaphoreType.REGULAR,
    ]
    mixed = pltpu.VMEM((width, rows), BF16)
    grad = pltpu.VMEM(w_gate.shape, BF16)
    results = pl.pallas_call(
        functools.partial(step_kernel, dims),
        out_shape=(mixed, grad, grad, grad),
        in_specs=[anywhere] * 7,
        out_specs=(pl.BlockSpec(memory_space=pltpu.VMEM),) * 4,
        scratch_shapes=scratch,
        compiler_params=pltpu.CompilerParams(
            collective_id=1, has_side_effects=True, vmem_limit_bytes=56 << 20
        ),
    )(tokens.T, cotangent.T, expert_ids.T, gate_weights.T, w_gate, w_up, w_down)
    mixed, gd, gg, gu = pl.pallas_call(
        store_kernel,
        out_shape=tuple(jax.ShapeDtypeStruct(r.shape, r.dtype) for r in results),
        in_specs=[pl.BlockSpec(memory_space=pltpu.VMEM)] * 4,
        out_specs=(anywhere,) * 4,
        scratch_shapes=[dma((4,))],
        compiler_params=pltpu.CompilerParams(vmem_limit_bytes=1 << 20),
    )(*[pltpu.with_memory_space_constraint(r, pltpu.VMEM) for r in results])
    return mixed.T, gg, gu, gd


def body(*args):
    if fits(args):
        return fused_layer(*args)
    return layer(*args)


def solution(mesh):
    rows = P(("expert", "dp"), None)
    mats = P("expert", "dp", None)
    return jax.shard_map(
        body,
        mesh=mesh,
        in_specs=(rows, rows, rows, rows, mats, mats, mats),
        out_specs=(rows, mats, mats, mats),
        check_vma=False,
    )
```

```python
import functools

import jax
import jax.numpy as jnp
from jax import lax
from jax.experimental import pallas as pl
from jax.experimental.pallas import tpu as pltpu
from jax.sharding import PartitionSpec as P


CAP = 512
INNER = 4
TILE = 768
PIECES = 2
HOPS = 2
STORES = 1
SWISH_SLOPE = 1.702
F32 = jnp.float32
BF16 = jnp.bfloat16


def dot(a, b):
    return jnp.dot(a, b, preferred_element_type=F32)


def dot_nt(a, b):
    return lax.dot_general(a, b, (((1,), (1,)), ((), ())), preferred_element_type=F32)


def dot_tn(a, b):
    return lax.dot_general(a, b, (((0,), (0,)), ((), ())), preferred_element_type=F32)


def share_kernel(size, x_ref, all_ref, send_sem, recv_sem):
    me = lax.axis_index("expert")
    barrier = pltpu.get_barrier_semaphore()
    for k in range(1, size):
        pl.semaphore_signal(
            barrier, inc=1, device_id={"expert": lax.rem(me + k, size)},
            device_id_type=pl.DeviceIdType.MESH,
        )
    pl.semaphore_wait(barrier, size - 1)
    copies = []
    for k in range(1, size):
        copy = pltpu.make_async_remote_copy(
            src_ref=x_ref, dst_ref=all_ref.at[me],
            send_sem=send_sem.at[k], recv_sem=recv_sem.at[k],
            device_id={"expert": lax.rem(me + k, size)},
            device_id_type=pl.DeviceIdType.MESH,
        )
        copy.start()
        copies.append(copy)
    all_ref[me] = x_ref[...]
    for copy in copies:
        copy.wait()


def share(x):
    size = lax.axis_size("expert")
    return pl.pallas_call(
        functools.partial(share_kernel, size),
        out_shape=jax.ShapeDtypeStruct((size,) + x.shape, x.dtype),
        in_specs=[pl.BlockSpec(memory_space=pltpu.VMEM)],
        out_specs=pl.BlockSpec(memory_space=pltpu.VMEM),
        scratch_shapes=[
            pltpu.SemaphoreType.DMA((size,)),
            pltpu.SemaphoreType.DMA((size,)),
        ],
        compiler_params=pltpu.CompilerParams(collective_id=0, has_side_effects=True),
    )(x)


def layer(tokens, cotangent, expert_ids, gate_weights, w_gate, w_up, w_down):
    size = lax.axis_size("expert")
    rows, top = expert_ids.shape
    width = tokens.shape[1]
    slot = 3 * rows * top // (2 * size)
    inner = min(INNER, size)
    outer = size // inner
    me = lax.axis_index("expert")
    mine_out, mine_in = me // inner, me % inner
    half = outer // 2
    partner = jnp.bitwise_xor(mine_in, jnp.arange(inner, dtype=jnp.int32))

    def shift(x, by):
        pairs = [(d, (d // inner + by) % outer * inner + d % inner) for d in range(size)]
        return lax.ppermute(x, "expert", pairs)

    def gather_outer(x):
        blocks = [x] + [None] * (outer - 1)
        for r in range(1, half + 1):
            if outer > 1:
                blocks[r] = shift(blocks[r - 1], 1)
        for r in range(1, outer - half):
            blocks[outer - r] = shift(blocks[(outer - r + 1) % outer], -1)
        return blocks

    def exchange(blocks):
        moved = list(blocks)
        for d in range(inner - 1, 0, -1):
            pairs = [(e, e // inner * inner + (e % inner ^ d)) for e in range(size)]
            moved[d] = lax.ppermute(blocks[d], "expert", pairs)
        return jnp.concatenate(moved)

    def relay(blocks):
        held = jnp.concatenate(blocks)
        return exchange([dot(part, held).astype(BF16) for part in select])

    meta = jnp.concatenate([expert_ids.T.astype(F32), gate_weights.T], axis=0)
    meta_all = share(meta)
    meta_all, tokens = lax.optimization_barrier((meta_all, tokens))
    token_blocks = gather_outer(tokens)
    token_blocks, cotangent = lax.optimization_barrier((token_blocks, cotangent))
    cot_blocks = gather_outer(cotangent)

    ids_all = meta_all[:, :top, :].astype(jnp.int32)
    gates_all = meta_all[:, top:, :]
    back = (mine_out - jnp.arange(outer, dtype=jnp.int32)) % outer

    before = (jnp.arange(rows)[:, None] < jnp.arange(rows)[None, :]).astype(BF16)

    ids_relay = jnp.stack([
        lax.dynamic_index_in_dim(ids_all, back[r] * inner + mine_in, 0, keepdims=False)
        for r in range(outer)
    ])
    near = mine_out * inner + partner
    named = jnp.any(ids_relay[None] == near[:, None, None, None], axis=2)
    rank = dot(named.astype(BF16).reshape(inner * outer, rows), before)
    rank = rank.reshape(inner, outer, rows).astype(jnp.int32)
    place = jnp.where(named, rank, slot)
    hit = place[:, :, None, :] == jnp.arange(slot, dtype=jnp.int32)[None, None, :, None]
    same = jnp.eye(outer, dtype=jnp.bool_)
    select = (hit[:, :, :, None, :] & same[None, :, None, :, None]).astype(BF16)
    select = select.reshape(inner, outer * slot, outer * rows)

    mask = jnp.any(ids_all == me, axis=1)
    gate_of = jnp.sum(jnp.where(ids_all == me, gates_all, 0.0), axis=1)
    counts = jnp.sum(mask.astype(jnp.int32), axis=1)
    below = jnp.arange(size)[:, None] > jnp.arange(size)[None, :]
    starts = jnp.sum(jnp.where(below, counts[None, :], 0), axis=1)
    own_rank = dot(mask.astype(BF16), before).astype(jnp.int32)
    position = jnp.where(mask, starts[:, None] + own_rank, CAP).reshape(1, size * rows)
    row_index = jnp.arange(CAP, dtype=jnp.int32)
    row_gate = jnp.sum(
        jnp.where(position == row_index[:, None], gate_of.reshape(1, size * rows), 0.0),
        axis=1, keepdims=True,
    )
    source = back[None, :] * inner + partner[:, None]
    is_source = source[:, :, None] == jnp.arange(size, dtype=jnp.int32)
    slot_start = jnp.sum(jnp.where(is_source, starts, 0), axis=2)
    slot_live = jnp.sum(jnp.where(is_source, counts, 0), axis=2)
    within = jnp.arange(slot, dtype=jnp.int32)
    slot_row = jnp.where(
        within < slot_live[:, :, None], slot_start[:, :, None] + within, CAP
    ).reshape(1, inner * outer * slot)
    pack = (row_index[:, None] == slot_row).astype(BF16)

    full_gate, full_up, full_down = (
        lax.all_gather(w_gate, "dp", axis=1, tiled=True)[0],
        lax.all_gather(w_up, "dp", axis=1, tiled=True)[0],
        lax.all_gather(w_down, "dp", axis=1, tiled=True)[0],
    )

    recv_x = relay(token_blocks)
    packed_x = dot(pack, recv_x).astype(BF16)
    pre_gate = dot(packed_x, full_gate)
    pre_up = dot(packed_x, full_up)
    sig = jax.nn.sigmoid(SWISH_SLOPE * pre_gate)
    value = pre_gate * sig
    slope = sig + SWISH_SLOPE * pre_gate * sig * (1.0 - sig)
    hidden = (value * (pre_up + 1.0)).astype(BF16)
    out = (dot_nt(hidden, full_down) * row_gate).astype(BF16)
    spread = dot_tn(pack, out).astype(BF16).reshape(inner, outer * slot, width)

    recv_g = relay(cot_blocks)
    spread, recv_g = lax.optimization_barrier((spread, recv_g))
    returned = exchange([spread[d] for d in range(inner)])
    packed_g = (dot(pack, recv_g) * row_gate).astype(BF16)
    grad_down = dot_tn(packed_g, hidden).astype(BF16)
    d_hidden = dot(packed_g, full_down)
    d_gate = (d_hidden * (pre_up + 1.0) * slope).astype(BF16)
    d_up = (d_hidden * value).astype(BF16)
    returned, d_gate, d_up = lax.optimization_barrier((returned, d_gate, d_up))
    partial = dot_tn(select.reshape(inner * outer * slot, outer * rows), returned)
    partial = partial.reshape(outer, rows, width)
    partial, d_gate, d_up = lax.optimization_barrier((partial, d_gate, d_up))
    grad_gate = dot_tn(packed_x, d_gate).astype(BF16)
    grad_up = dot_tn(packed_x, d_up).astype(BF16)

    total = partial[0]
    ahead = partial[half]
    behind = partial[half + 1] if outer - half > 1 else None
    for r in range(half - 1, -1, -1):
        ahead = shift(ahead.astype(BF16), -1).astype(F32)
        if r > 0:
            ahead = ahead + partial[r]
    for r in range(half + 2, outer + 1):
        behind = shift(behind.astype(BF16), 1).astype(F32)
        if r < outer:
            behind = behind + partial[r]
    if half > 0:
        total = total + ahead
    if behind is not None:
        total = total + behind
    mixed = total.astype(BF16)

    grads = [
        lax.psum_scatter(g, "dp", scatter_dimension=0, tiled=True)[None]
        for g in (grad_down, grad_gate, grad_up)
    ]
    return mixed, grads[1], grads[2], grads[0]


def flip(i, d):
    out, bit = 0, 1
    while bit <= max(d, INNER - 1):
        out = out + lax.rem(lax.rem(i // bit, 2) + (d // bit) % 2, 2) * bit
        bit *= 2
    return out


def step_kernel(
    dims, tok_in, cot_in, ids_in, gates_in, wg_in, wu_in, wd_in,
    mixed_out, gd_out, gg_out, gu_out,
    ids_buf, gates_buf, col, meta, sel, selg, send, send_t, recv, recv_t, back, back_t, pack, packg,
    x, act, out, out_t, g, coef, w, xt, dact,
    zin, zout, near, mask, gq, start, count, place, row_gate, total, mixed,
    load_sem, z_send, z_recv, m_send, m_recv, ms_send, ms_recv, p_send, p_recv,
    w_send, w_recv, r_send, r_recv, g_send, g_recv, free_sem, o_sem,
):
    size, outer, inner, rows, width, top, slot, shard = dims
    main = width // 128 * 128
    rest = width - main
    groups = slot // 16
    few = inner * 16
    span = inner * slot
    me = lax.axis_index("expert")
    dp = lax.axis_index("dp")
    mo, mi = me // inner, lax.rem(me, inner)
    pal = [flip(mi, d) + mo * inner for d in range(inner)]
    other = 1 - dp
    has_up, has_dn = mo < outer - 1, mo > 0
    mesh_id = pl.DeviceIdType.MESH

    def remote(src, dst, ss, rs, device):
        return pltpu.make_async_remote_copy(
            src_ref=src, dst_ref=dst, send_sem=ss, recv_sem=rs,
            device_id=device, device_id_type=mesh_id,
        )

    def tiles(fn, end=width):
        full = end // TILE
        if full:
            def step(i, carry):
                fn(pl.ds(pl.multiple_of(i * TILE, TILE), TILE))
                return carry

            lax.fori_loop(0, full, step, 0)
        if end % TILE:
            fn(pl.ds(full * TILE, end % TILE))

    def repeat(t):
        return jnp.concatenate([t] * (128 // rest), axis=0)

    def lane_group(count, g):
        lane = lax.broadcasted_iota(jnp.int32, (count, 128), 1)
        return jnp.logical_and(lane >= g * rest, lane < (g + 1) * rest)

    def fold(y, count):
        out_rows = jnp.zeros((count, 128), F32)
        for g in range(groups):
            out_rows = jnp.where(lane_group(count, g), y[g * count:(g + 1) * count, :], out_rows)
        return out_rows.astype(BF16)

    def zero_ends():
        for way, has in ((0, has_up), (1, has_dn)):
            @pl.when(jnp.logical_not(has))
            def _():
                zin[way, 0] = jnp.zeros((width, rows), BF16)

    own_rows = pl.ds(pl.multiple_of(dp * shard, 16), shard)
    loads = [
        pltpu.make_async_copy(tok_in, col.at[0, mo], load_sem.at[0]),
        pltpu.make_async_copy(cot_in, col.at[1, mo], load_sem.at[1]),
        pltpu.make_async_copy(ids_in, ids_buf, load_sem.at[2]),
        pltpu.make_async_copy(gates_in, gates_buf, load_sem.at[6]),
    ]
    w_ins = (wd_in, wg_in, wu_in)
    w_loads = [
        pltpu.make_async_copy(w_ins[k].at[0], w.at[k, own_rows], load_sem.at[3 + k])
        for k in range(3)
    ]
    for c in loads + w_loads:
        c.start()

    barrier = pltpu.get_barrier_semaphore()
    for d in range(1, inner):
        pl.semaphore_signal(barrier, inc=1, device_id={"expert": pal[d]}, device_id_type=mesh_id)
    pl.semaphore_signal(barrier, inc=1, device_id={"dp": other}, device_id_type=mesh_id)

    @pl.when(has_up)
    def _():
        pl.semaphore_signal(barrier, inc=1, device_id={"expert": me + inner}, device_id_type=mesh_id)

    @pl.when(has_dn)
    def _():
        pl.semaphore_signal(barrier, inc=1, device_id={"expert": me - inner}, device_id_type=mesh_id)

    zero_ends()
    for c in loads[2:]:
        c.wait()
    meta[mo, 0, 0:top, :] = ids_buf[...].astype(F32)
    meta[mo, 0, top:2 * top, :] = gates_buf[...]
    for c in loads[:2]:
        c.wait()
    pl.semaphore_wait(
        barrier, inner + has_up.astype(jnp.int32) + has_dn.astype(jnp.int32)
    )


    def piece(h):
        return pl.ds(h * (width // PIECES), width // PIECES)

    def z_copy(kind, way, r, h=0):
        b = mo - r if way == 0 else mo + r
        to = me + inner if way == 0 else me - inner
        if kind == 2:
            return remote(meta.at[b, 0], meta.at[b, 0], ms_send.at[way, r], ms_recv.at[way, r], {"expert": to})
        part = col.at[kind, b, piece(h)]
        return remote(part, part, z_send.at[kind, way, r, h], z_recv.at[kind, way, r, h], {"expert": to})

    def sends_z(way, r):
        if way == 0:
            return jnp.logical_and(mo >= r, has_up)
        return jnp.logical_and(mo + r < outer, has_dn)

    def gets_z(way, r):
        return mo >= r + 1 if way == 0 else mo + r + 1 < outer

    def z_wait(kind, way, r, h=0):
        b = mo - 1 - r if way == 0 else mo + 1 + r
        frm = me - inner if way == 0 else me + inner
        if kind == 2:
            remote(meta.at[b, 0], meta.at[b, 0], ms_send.at[way, r], ms_recv.at[way, r], {"expert": frm}).wait_recv()
        else:
            part = col.at[kind, b, piece(h)]
            remote(
                part, part, z_send.at[kind, way, r, h], z_recv.at[kind, way, r, h], {"expert": frm}
            ).wait_recv()

    def z_issue(kind, way, r, h):
        @pl.when(sends_z(way, r))
        def _():
            if kind == 0 and h == 0:
                z_copy(2, way, r).start()
            z_copy(kind, way, r, h).start()
            if kind == 0 and h == PIECES - 1:
                last = mo == r if way == 0 else mo + r == outer - 1

                @pl.when(last)
                def _():
                    for i in range(PIECES):
                        z_copy(1, way, 0, i).start()

    def z_round(kind, r):
        for h in range(PIECES):
            for way in (0, 1):
                @pl.when(gets_z(way, r))
                def _():
                    if kind == 0 and h == 0:
                        z_wait(2, way, r)
                    z_wait(kind, way, r, h)
                    if r + 1 < outer - 1:
                        z_issue(kind, way, r + 1, h)

    for h in range(PIECES):
        for way in (0, 1):
            z_issue(0, way, 0, h)

    def w_copy(k):
        return remote(w_ins[k].at[0], w.at[k, own_rows], w_send.at[k], w_recv.at[k], {"dp": other})

    for k in (1, 2, 0):
        w_copy(k).start()

    sub = lax.broadcasted_iota(jnp.int32, (8, rows), 0)
    wanted = jnp.full((8, rows), -7, jnp.int32)
    for d in range(inner):
        wanted = jnp.where(sub == d, pal[d], wanted)
    near[...] = wanted.astype(F32)

    def earlier():
        a = lax.broadcasted_iota(jnp.int32, (rows, rows), 0)
        b = lax.broadcasted_iota(jnp.int32, (rows, rows), 1)
        return jnp.where(a < b, 1.0, 0.0).astype(BF16)

    def build(b):
        ids = meta[b, 0]
        named = jnp.zeros((8, rows), F32)
        for k in range(top):
            named = named + jnp.where(ids[k:k + 1, :] == near[...], 1.0, 0.0)
        rank = dot(named.astype(BF16), earlier())
        spot = jnp.where(named > 0.0, rank, float(slot))
        within = lax.broadcasted_iota(jnp.int32, (slot, rows), 0).astype(F32)
        for d in range(inner):
            hit = jnp.where(spot[d:d + 1, :] == within, 1.0, 0.0).astype(BF16)
            sel[b, d * slot:(d + 1) * slot, :] = hit
            for i in range(groups):
                selg[b, i * few + d * 16:i * few + (d + 1) * 16, :] = hit[i * 16:(i + 1) * 16, :]

    def m_copy(b, d):
        return remote(meta.at[b, 0], meta.at[b, d], m_send.at[b, d], m_recv.at[b, d], {"expert": pal[d]})

    def p_copy(kind, b, d):
        part, little = pl.ds(d * slot, slot), pl.ds(d * 16, 16)
        to = {"expert": pal[d]}
        frm = kind if kind < 2 else 0
        ends = (recv.at[kind, b, part], recv_t.at[kind, b, little]) if kind < 2 else (
            back.at[b, part], back_t.at[b, little])
        return (
            remote(send.at[frm, b, part], ends[0], p_send.at[kind, b, d, 0], p_recv.at[kind, b, d, 0], to),
            remote(send_t.at[frm, b, little], ends[1], p_send.at[kind, b, d, 1], p_recv.at[kind, b, d, 1], to),
        )

    def p_start(kind, b, d):
        for c in p_copy(kind, b, d):
            c.start()

    def p_wait_recv(kind, b, d):
        for c in p_copy(kind, b, d):
            c.wait_recv()

    def p_wait_send(kind, b, d):
        for c in p_copy(kind, b, d):
            c.wait_send()

    def scatter(kind, b):
        picked = dot_nt(sel[b], col[kind, b, :main, :]).astype(BF16)
        picked_t = fold(dot_nt(selg[b], repeat(col[kind, b, main:, :])), few)
        send[kind, b, slot:, :] = picked[slot:, :]
        send_t[kind, b, 16:, :] = picked_t[16:, :]
        recv[kind, b, :slot, :] = picked[:slot, :]
        recv_t[kind, b, :16, :] = picked_t[:16, :]
        for d in range(1, inner):
            p_start(kind, b, d)

    def spread_tok(b):
        for d in range(1, inner):
            m_copy(b, d).start()
        build(b)
        scatter(0, b)

    spread_tok(mo)
    scatter(1, mo)
    for r in range(outer - 1):
        z_round(0, r)
        for way in (0, 1):
            @pl.when(gets_z(way, r))
            def _():
                spread_tok(mo - 1 - r if way == 0 else mo + 1 + r)

    at_end = jnp.logical_or(mo == 0, mo == outer - 1)
    inside = jnp.logical_not(at_end)

    def cot_round(r):
        z_round(1, r)
        for way in (0, 1):
            @pl.when(gets_z(way, r))
            def _():
                scatter(1, mo - 1 - r if way == 0 else mo + 1 + r)

    def cot_at(r, when):
        if r < outer - 1:
            @pl.when(when)
            def _():
                cot_round(r)

    for b in range(outer):
        for d in range(1, inner):
            m_copy(b, d).wait_recv()
    mine = jnp.full((1, rows), me, jnp.int32).astype(F32)
    for b in range(outer):
        for d in range(inner):
            q = b * inner + d
            row, gate = jnp.zeros((1, rows), F32), jnp.zeros((1, rows), F32)
            for k in range(top):
                same = meta[b, d, k:k + 1, :] == mine
                row = row + jnp.where(same, 1.0, 0.0)
                gate = gate + jnp.where(same, meta[b, d, top + k:top + k + 1, :], 0.0)
            mask[q:q + 1, :] = row
            gq[q:q + 1, :] = gate
    held = mask[...].astype(BF16)
    first = jnp.bitwise_xor(lax.broadcasted_iota(jnp.int32, (size, size), 0), mi)
    second = jnp.bitwise_xor(lax.broadcasted_iota(jnp.int32, (size, size), 1), mi)
    order = jnp.where(second < first, 1.0, 0.0).astype(BF16)
    ones = jnp.ones((rows, rows), BF16)
    begin = dot(dot(order, held).astype(BF16), ones)
    start[...] = begin
    count[...] = dot(held, ones)
    place[...] = jnp.where(mask[...] > 0.0, begin + dot(held, earlier()), float(CAP))
    within = lax.broadcasted_iota(jnp.int32, (slot, 128), 0).astype(F32)
    lane = lax.broadcasted_iota(jnp.int32, (slot, 128), 1).astype(F32)
    for q in range(size):
        target = jnp.where(within < count[q:q + 1, :128], start[q:q + 1, :128] + within, float(CAP))
        for j in range(CAP // 128):
            hit = jnp.where(target == lane + float(j * 128), 1.0, 0.0).astype(BF16)
            here = slice(j * 128, (j + 1) * 128)
            pack[q * slot:(q + 1) * slot, here] = hit
            b, d = q // inner, q % inner
            for i in range(groups):
                packg[i, b, d * 16:(d + 1) * 16, here] = hit[i * 16:(i + 1) * 16, :]
    down = lax.broadcasted_iota(jnp.int32, (128, rows), 0).astype(F32)
    for j in range(CAP // 128):
        acc = jnp.zeros((128, rows), F32)
        for q in range(size):
            acc = acc + jnp.where(place[q:q + 1, :] == down + float(j * 128), gq[q:q + 1, :], 0.0)
        row_gate[j * 128:(j + 1) * 128, :] = jnp.broadcast_to(jnp.sum(acc, axis=1, keepdims=True), (128, 128))

    low = jnp.logical_not(mo * 2 < outer).astype(jnp.int32)
    last = (1 - low) * (outer - 1)

    def arrive(kind, begin, n_blocks):
        for i in range(n_blocks):
            for d in range(1, inner):
                p_wait_recv(kind, begin + i, d)

    def gather(kind, begin, n_blocks, n):
        from_rows = pl.ds(pl.multiple_of(begin * span, 16), n_blocks * span)
        blocks = recv[kind, pl.ds(begin, n_blocks), :, n]
        return dot_tn(pack[from_rows, :], blocks.reshape(n_blocks * span, n.size))

    def gather_t(kind, begin, n_blocks):
        n_few = n_blocks * few
        held_t = recv_t[kind, pl.ds(begin, n_blocks)].reshape(n_few, 128).astype(F32)
        wide = jnp.zeros((CAP, 128), F32)
        for i in range(groups):
            one = jnp.where(lane_group(n_few, i), held_t, 0.0).astype(BF16)
            wide = wide + dot_tn(packg[i, pl.ds(begin, n_blocks)].reshape(n_few, CAP), one)
        thin = wide[:, :rest]
        for i in range(1, groups):
            thin = thin + wide[:, i * rest:(i + 1) * rest]
        return thin

    def fill(kind, ref, gated):
        def finish(v):
            return (v * row_gate[:, :1] if gated else v).astype(BF16)

        def early(n):
            ref[:, n] = finish(gather(kind, low, outer - 1, n))

        def late(n):
            ref[:, n] = ref[:, n] + finish(gather(kind, last, 1, n))

        def early_all():
            tiles(early, main)
            ref[:, main:] = finish(gather_t(kind, low, outer - 1))

        def late_all():
            tiles(late, main)
            ref[:, main:] = ref[:, main:] + finish(gather_t(kind, last, 1))

        return early_all, late_all

    x_early, x_late = fill(0, x, False)
    g_early, g_late = fill(1, g, True)
    cot_at(0, inside)
    arrive(0, low, outer - 1)
    x_early()
    arrive(0, last, 1)
    cot_at(0, at_end)
    x_late()
    cot_at(1, inside)

    for k in (1, 2):
        w_loads[k].wait()
        w_copy(k).wait_recv()

    def forward(n):
        pre_gate = dot(x[...], w[1, :, n])
        pre_up = dot(x[...], w[2, :, n]) + 1.0
        sig = jax.nn.sigmoid(SWISH_SLOPE * pre_gate)
        value = pre_gate * sig
        slope = sig + SWISH_SLOPE * value * (1.0 - sig)
        act[:, n] = (value * pre_up).astype(BF16)
        coef[0, :, n] = pre_up * slope
        coef[1, :, n] = value

    tiles(forward)
    pl.semaphore_signal(free_sem.at[0], inc=1, device_id={"dp": other}, device_id_type=mesh_id)
    cot_at(1, at_end)

    w_loads[0].wait()
    w_copy(0).wait_recv()

    def project(n):
        out[:, n] = (dot_nt(act[...], w[0, n, :]) * row_gate[:, :1]).astype(BF16)

    tiles(project, main)
    out_t[...] = (dot_nt(act[...], repeat(w[0, main:, :])) * row_gate[:, :1]).astype(BF16)
    for b in range(outer):
        for d in range(1, inner):
            p_wait_send(0, b, d)


    def give_back(b):
        part = pl.ds(pl.multiple_of(b * span, 16), span)
        rows_back = dot(pack[part, :], out[...]).astype(BF16)
        rows_t = fold(dot(packg[:, b].reshape(groups * few, CAP), out_t[...]), few)
        send[0, b, slot:, :] = rows_back[slot:, :]
        send_t[0, b, 16:, :] = rows_t[16:, :]
        back[b, :slot, :] = rows_back[:slot, :]
        back_t[b, :16, :] = rows_t[:16, :]
        for d in range(1, inner):
            p_start(2, b, d)

    def give_round(r):
        @pl.when(mo >= r)
        def _():
            give_back(mo - r)

        if r > 0:
            @pl.when(mo + r < outer)
            def _():
                give_back(mo + r)

    give_round(outer - 1)
    for r in range(2, outer - 1):
        cot_round(r)

    @pl.when(inside)
    def _():
        for r in range(outer - 2, -1, -1):
            give_round(r)


    def strip(h):
        return pl.ds(h * (width // HOPS), width // HOPS)

    def r_copy(way, r, h):
        to = me - inner if way == 0 else me + inner
        return remote(
            zout.at[way, r - 1, strip(h)], zin.at[way, r - 1, strip(h)],
            r_send.at[way, r - 1, h], r_recv.at[way, r - 1, h], {"expert": to},
        )

    def partial(b):
        for d in range(1, inner):
            p_wait_recv(2, b, d)
        thin = jnp.zeros((rest, rows), F32)
        for i in range(groups):
            thin = thin + dot_tn(back_t[b], selg[b, i * few:(i + 1) * few, :])[i * rest:(i + 1) * rest, :]
        return jnp.concatenate([dot_tn(back[b], sel[b]), thin], axis=0)

    def gives(way, r):
        return mo >= r if way == 0 else mo + r < outer

    def ret_round(r):
        for way in (0, 1):
            @pl.when(gives(way, r))
            def _():
                zout[way, r - 1] = partial(mo - r if way == 0 else mo + r).astype(BF16)
        for h in range(HOPS):
            for way, inbound in ((0, has_up), (1, has_dn)):
                @pl.when(gives(way, r))
                def _():
                    if r < outer - 1:
                        @pl.when(inbound)
                        def _():
                            r_copy(way, r + 1, h).wait_recv()
                            zout[way, r - 1, strip(h)] = (
                                zout[way, r - 1, strip(h)].astype(F32) + zin[way, r, strip(h)].astype(F32)
                            ).astype(BF16)
                    r_copy(way, r, h).start()

    def ret_last():
        total[...] = partial(mo)
        for b in range(outer):
            for d in range(1, inner):
                p_wait_send(2, b, d)
        for k in range(3):
            g_copy(k).wait_send()
        for h in range(HOPS):
            for way, inbound in ((0, has_up), (1, has_dn)):
                @pl.when(inbound)
                def _():
                    r_copy(way, 1, h).wait_recv()
            mixed[strip(h)] = (
                total[strip(h)] + zin[0, 0, strip(h)].astype(F32) + zin[1, 0, strip(h)].astype(F32)
            ).astype(BF16)

    def flip_x(n):
        xt[1, n, :] = dot_tn(x[:, n], unit()).astype(BF16)

    def unit():
        a = lax.broadcasted_iota(jnp.int32, (CAP, CAP), 0)
        b = lax.broadcasted_iota(jnp.int32, (CAP, CAP), 1)
        return jnp.where(a == b, 1.0, 0.0).astype(BF16)

    tiles(flip_x)
    arrive(1, low, outer - 1)
    g_early()
    ret_round(outer - 1)

    @pl.when(at_end)
    def _():
        for r in range(outer - 2, -1, -1):
            give_round(r)

    for way in (0, 1):
        for r in range(outer - 1):
            @pl.when(sends_z(way, r))
            def _():
                z_copy(2, way, r).wait_send()
                for h in range(PIECES):
                    z_copy(0, way, r, h).wait_send()
                    z_copy(1, way, r, h).wait_send()
    for k in range(3):
        w_copy(k).wait_send()
    for b in range(outer):
        for d in range(1, inner):
            m_copy(b, d).wait_send()
    for i in range(outer - 1):
        for d in range(1, inner):
            p_wait_send(1, low + i, d)
    arrive(1, last, 1)
    for d in range(1, inner):
        p_wait_send(1, last, d)

    g_late()

    def flip_g(n):
        xt[0, n, :] = dot_tn(g[:, n], unit()).astype(BF16)

    tiles(flip_g)

    spot_of = (1, 2, 0)
    send_rows = pl.ds(0, shard)
    recv_rows = pl.ds(shard, shard)

    def g_copy(k):
        return remote(
            w.at[spot_of[k], send_rows], w.at[spot_of[k], recv_rows], g_send.at[k], g_recv.at[k], {"dp": other}
        )

    def right(k, n):
        return act[:, n] if k == 0 else dact[k - 1, :, n]

    their_rows = pl.ds(pl.multiple_of(other * shard, 16), shard)

    def send_theirs(k):
        def theirs(n):
            w[spot_of[k], send_rows, n] = dot(xt[min(k, 1), their_rows, :], right(k, n)).astype(BF16)

        tiles(theirs)
        g_copy(k).start()

    pl.semaphore_wait(free_sem.at[0], 1)
    send_theirs(0)

    def back_act(n):
        d_hidden = dot(g[...], w[0, :, n])
        dact[0, :, n] = (d_hidden * coef[0, :, n]).astype(BF16)
        dact[1, :, n] = (d_hidden * coef[1, :, n]).astype(BF16)

    tiles(back_act)
    pl.semaphore_signal(free_sem.at[1], inc=1, device_id={"dp": other}, device_id_type=mesh_id)

    for r in range(outer - 2, 1, -1):
        ret_round(r)
    send_theirs(1)
    pl.semaphore_wait(free_sem.at[1], 1)
    send_theirs(2)
    if outer > 2:
        ret_round(1)
    outs = (gd_out, gg_out, gu_out)
    stores = []
    for k in range(3):
        lhs = 0 if k == 0 else 1
        g_copy(k).wait_recv()

        def ours(n):
            grad = dot(xt[lhs, own_rows, :], right(k, n)) + w[spot_of[k], recv_rows, n].astype(F32)
            w[spot_of[k], recv_rows, n] = grad.astype(BF16)

        tiles(ours)
        store = pltpu.make_async_copy(w.at[spot_of[k], recv_rows], outs[k].at[0], o_sem.at[k])
        store.start()
        stores.append(store)
    ret_last()
    stores.append(pltpu.make_async_copy(mixed, mixed_out, o_sem.at[3]))
    stores[3].start()

    for way in (0, 1):
        for r in range(1, outer):
            @pl.when(gives(way, r))
            def _():
                for h in range(HOPS):
                    r_copy(way, r, h).wait_send()
    for store in stores:
        store.wait()


def store_kernel(*refs):
    sem = refs[-1]
    copies = []
    for k in range(4):
        src, dst = refs[k], refs[4 + k]
        if k > 0:
            src, dst = src.at[0], dst.at[0]
        step = src.shape[0] // STORES
        for i in range(STORES):
            part = pl.ds(i * step, step)
            copies.append(pltpu.make_async_copy(src.at[part], dst.at[part], sem.at[k, i]))
    for c in copies:
        c.start()
    for c in copies:
        c.wait()


def slots(args):
    rows, top = args[2].shape
    return -(-3 * rows * top // (2 * lax.axis_size("expert")) // 16) * 16


def fits(args):
    rows, width = args[0].shape
    shard = args[4].shape[1]
    size = lax.axis_size("expert")
    return (
        lax.axis_size("dp") == 2 and args[2].shape[1] == 4 and shard % 16 == 0 and rows == 128
        and size % INNER == 0 and INNER < size <= 16
        and width % 128 in (32, 64) and slots(args) // 16 * (width % 128) <= 128
    )


def fused_layer(tokens, cotangent, expert_ids, gate_weights, w_gate, w_up, w_down):
    size = lax.axis_size("expert")
    rows, top = expert_ids.shape
    width = tokens.shape[1]
    shard = w_gate.shape[1]
    hid = w_gate.shape[2]
    inner = INNER
    outer = size // inner
    slot = slots((tokens, cotangent, expert_ids))
    span = inner * slot
    main, few = width // 128 * 128, inner * 16
    dims = (size, outer, inner, rows, width, top, slot, shard)
    anywhere = pl.BlockSpec(memory_space=pl.ANY)
    dma = pltpu.SemaphoreType.DMA
    hop = outer - 1
    scratch = [
        pltpu.VMEM((top, rows), jnp.int32),
        pltpu.VMEM((top, rows), F32),
        pltpu.VMEM((2, outer, width, rows), BF16),
        pltpu.VMEM((outer, inner, 2 * top, rows), F32),
        pltpu.VMEM((outer, span, rows), BF16),
        pltpu.VMEM((outer, span, rows), BF16),
        pltpu.VMEM((2, outer, span, main), BF16),
        pltpu.VMEM((2, outer, few, 128), BF16),
        pltpu.VMEM((2, outer, span, main), BF16),
        pltpu.VMEM((2, outer, few, 128), BF16),
        pltpu.VMEM((outer, span, main), BF16),
        pltpu.VMEM((outer, few, 128), BF16),
        pltpu.VMEM((outer * span, CAP), BF16),
        pltpu.VMEM((slot // 16, outer, few, CAP), BF16),
        pltpu.VMEM((CAP, width), BF16),
        pltpu.VMEM((CAP, hid), BF16),
        pltpu.VMEM((CAP, main), BF16),
        pltpu.VMEM((CAP, 128), BF16),
        pltpu.VMEM((CAP, width), BF16),
        pltpu.VMEM((2, CAP, hid), F32),
        pltpu.VMEM((3, 2 * shard, hid), BF16),
        pltpu.VMEM((2, width, CAP), BF16),
        pltpu.VMEM((2, CAP, hid), BF16),
        pltpu.VMEM((2, hop, width, rows), BF16),
        pltpu.VMEM((2, hop, width, rows), BF16),
        pltpu.VMEM((8, rows), F32),
        pltpu.VMEM((size, rows), F32),
        pltpu.VMEM((size, rows), F32),
        pltpu.VMEM((size, rows), F32),
        pltpu.VMEM((size, rows), F32),
        pltpu.VMEM((size, rows), F32),
        pltpu.VMEM((CAP, 128), F32),
        pltpu.VMEM((width, rows), F32),
        pltpu.VMEM((width, rows), BF16),
        dma((7,)), dma((2, 2, hop, PIECES)), dma((2, 2, hop, PIECES)),
        dma((outer, inner)), dma((outer, inner)), dma((2, hop)), dma((2, hop)),
        dma((3, outer, inner, 2)), dma((3, outer, inner, 2)),
        dma((3,)), dma((3,)), dma((2, hop, HOPS)), dma((2, hop, HOPS)), dma((3,)), dma((3,)),
        pltpu.SemaphoreType.REGULAR((2,)), dma((4,)),
    ]
    mixed = pltpu.VMEM((width, rows), BF16)
    grad = pltpu.VMEM(w_gate.shape, BF16)
    results = pl.pallas_call(
        functools.partial(step_kernel, dims),
        out_shape=(mixed, grad, grad, grad),
        in_specs=[anywhere] * 7,
        out_specs=(anywhere,) * 4,
        scratch_shapes=scratch,
        compiler_params=pltpu.CompilerParams(
            collective_id=1, has_side_effects=True, vmem_limit_bytes=56 << 20
        ),
    )(tokens.T, cotangent.T, expert_ids.T, gate_weights.T, w_gate, w_up, w_down)
    mixed, gd, gg, gu = pl.pallas_call(
        store_kernel,
        out_shape=tuple(jax.ShapeDtypeStruct(r.shape, r.dtype) for r in results),
        in_specs=[pl.BlockSpec(memory_space=pltpu.VMEM)] * 4,
        out_specs=(anywhere,) * 4,
        scratch_shapes=[dma((4, STORES))],
        compiler_params=pltpu.CompilerParams(vmem_limit_bytes=1 << 20),
    )(*[pltpu.with_memory_space_constraint(r, pltpu.VMEM) for r in results])
    return mixed.T, gg, gu, gd


def body(*args):
    if fits(args):
        return fused_layer(*args)
    return layer(*args)


def solution(mesh):
    rows = P(("expert", "dp"), None)
    mats = P("expert", "dp", None)
    return jax.shard_map(
        body,
        mesh=mesh,
        in_specs=(rows, rows, rows, rows, mats, mats, mats),
        out_specs=(rows, mats, mats, mats),
        check_vma=False,
    )
```
